256 devices in a mesh: energy: 64 (over y, x_lo, z), layer: 4 (over x_hi, core).
Axes of the slice: x: 4 (x_hi: 2, x_lo: 2; x = x_hi * 2 + x_lo), y: 4, z: 8, core: 2. Of those that a mesh axis runs over, the one named last changes fastest.
Arguments:
- layer_inverse: float32 [64, 32, 256, 256], P('energy', 'layer'), may hold values from -0.008125 to 1, as said below
- coupling: float32 [256, 256], replicated, may hold values from -0.5125 to 0.5125, as said below
- lead_left: float32 [64, 256, 256], P('energy'), may hold values from -0.0040625 to 0.5, as said below
- lead_right: float32 [64, 256, 256], P('energy'), may hold values from -0.0040625 to 0.5, as said below
- quad_weight: float32 [64], replicated, may hold values from 0.0015625 to 0.0625
- energy_slot: int32 [64], P('energy'), may hold values from 0 to 63, each once
- plane_of: int32 [32], replicated, may hold values from 0 to 1023
- doping: float32 [1024, 128, 128], P(('energy', 'layer')), may hold values from -6 to 6
- screening: float32 [1024, 128, 128], P(('energy', 'layer')), may hold values from 0.25 to 2
Outputs:
- layer_density: float32 [32, 256], P('layer')
- potential: float32 [1024, 128, 128], P(('energy', 'layer'))
- residual: float32 [1024, 128, 128], P(('energy', 'layer'))
The draws below stay inside these ranges and needn't reach their ends.
Inputs may be any that keep to these rules, and one draw needn't show every extreme that they name: `layer_inverse`: each block is symmetric; its diagonal entries lie between 0.3 and 1.0 and its other entries within 0.13 * 256 ** -0.5 of zero. `coupling`: entries are independent with mean zero. `lead_left`: each block is symmetric; its diagonal entries lie between 0.15 and 0.5 and its other entries within 0.065 * 256 ** -0.5 of zero. `lead_right`: each block is symmetric; its diagonal entries lie between 0.15 and 0.5 and its other entries within 0.065 * 256 ** -0.5 of zero. `energy_slot`: every quadrature index appears once. `plane_of`: several layers may share a plane.
All inputs are finite; a program needn't handle non-finite values.
Results may differ from the reference program's by a relative error of at most 0.00018.
Values sent between devices are 32-bit elements; how exact they have to be, the bound alone decides.
A program may use at most 128 MiB of HBM per device.

```python
import math
from functools import partial
import jax
import jax.numpy as jnp
from jax import lax

M = 256
ORB_Y = 16
ORB_Z = 16
NY = 128
NZ = 128
LAYERS = 32
ENERGIES = 64
NX = 1024
CG_ITERS = 3


def symmetric_blocks(key, lead_shape, factor):
    key_diag, key_off = jax.random.split(key)
    orbitals = M
    diag_values = jnp.exp(jax.random.uniform(key_diag, lead_shape + (orbitals,), jnp.float32, math.log(0.3), 0.0))
    half_width = 0.13 * orbitals ** (-0.5)
    noise = jax.random.uniform(key_off, lead_shape + (orbitals, orbitals), jnp.float32, -half_width, half_width)
    noise = 0.5 * (noise + jnp.swapaxes(noise, -1, -2))
    identity_mat = jnp.eye(orbitals, dtype=jnp.float32)
    blocks = noise * (1.0 - identity_mat) + diag_values[..., None] * identity_mat
    return (factor * blocks).astype(jnp.float32)


def draw_layer_inverse(key, part):
    return symmetric_blocks(jax.random.fold_in(key, 11), (ENERGIES, LAYERS), 1.0)


def draw_coupling(key, part):
    coupling_key = jax.random.fold_in(key, 14)
    spread = 1.36 * M ** (-0.5)
    values = jnp.clip(spread * jax.random.normal(coupling_key, (M, M), jnp.float32), -6.0 * spread, 6.0 * spread)
    return values.astype(jnp.float32)


def draw_lead_left(key, part):
    return symmetric_blocks(jax.random.fold_in(key, 12), (ENERGIES,), 0.5)


def draw_lead_right(key, part):
    return symmetric_blocks(jax.random.fold_in(key, 13), (ENERGIES,), 0.5)


def set_ends(drawn, rng, least, top_value):
    longest = drawn.shape.index(max(drawn.shape))
    spots = []
    for shift in (0, 1):
        where = [jax.random.randint(jax.random.fold_in(rng, axis), (), 0, length) for axis, length in enumerate(drawn.shape)]
        where[longest] = (where[longest] + shift) % drawn.shape[longest]
        spots.append(tuple(where))
    return drawn.at[spots[0]].set(least).at[spots[1]].set(top_value)


def shard_levels(key, shape, pieces, low, top_value):
    gain, own = 1.0, jax.random.fold_in(key, 6)
    for position, shards_of in pieces:
        steps = jnp.exp(jax.random.uniform(jax.random.fold_in(own, position), (shards_of,), jnp.float32, low / len(pieces), top_value / len(pieces)))
        gain = gain * jnp.repeat(steps, shape[position] // shards_of).reshape([-1 if axis == position else 1 for axis in range(len(shape))])
    return gain


def gaussian(key, shape, deviation, most, cuts=(), kind=jnp.bfloat16):
    array = jax.random.normal(key, shape, jnp.float32) * deviation
    if len(cuts) > 0:
        array = shard_levels(key, shape, cuts, -0.22, 0.18) * array
    return jnp.clip(array, min=-most, max=most).astype(kind)


def setup_inputs(seed: int = 0) -> dict:
    splits = jax.random.split(jax.random.key(seed), 10)
    return {
        "layer_inverse": draw_layer_inverse(jax.random.fold_in(splits[9], 71), 0),
        "coupling": draw_coupling(jax.random.fold_in(splits[9], 71), 0),
        "lead_left": draw_lead_left(jax.random.fold_in(splits[9], 71), 0),
        "lead_right": draw_lead_right(jax.random.fold_in(splits[9], 71), 0),
        "quad_weight": jnp.clip(jnp.exp(jax.random.uniform(splits[4], (ENERGIES,), jnp.float32, math.log(0.0015625), math.log(0.0625))), 0.0015625, 0.0625),
        "energy_slot": jax.random.permutation(splits[5], ENERGIES).astype(jnp.int32),
        "plane_of": set_ends(jax.random.randint(splits[6], (LAYERS,), 0, NX), jax.random.fold_in(splits[6], 1), 0, NX - 1).astype(jnp.int32),
        "doping": gaussian(splits[7], (NX, NY, NZ), 1.0, 6.0, ((0, 256),), jnp.float32),
        "screening": jnp.clip(0.25 + 1.75 * jax.random.uniform(splits[8], (NX, NY, NZ), jnp.float32) ** shard_levels(splits[8], (NX, NY, NZ), ((0, 256),), -0.2, 0.2), 0.25, 2.0),
    }


exact_mode = lax.Precision.HIGHEST


def matmul_hi(left_mat, right_mat):
    return jnp.matmul(left_mat, right_mat, precision=exact_mode)


def chain_diagonals(tmat, energy_item):
    inverse, left_lead, right_lead = energy_item
    forward = matmul_hi(inverse, tmat)
    backward = matmul_hi(inverse, tmat.T)

    def step_chain(state_mat, layer_pair):
        inv_layer, propagator = layer_pair
        following = inv_layer + matmul_hi(matmul_hi(propagator, state_mat), propagator.T)
        return following, state_mat

    _, left_in = lax.scan(step_chain, left_lead, (inverse, forward))
    _, right_in = lax.scan(step_chain, right_lead, (inverse, backward), reverse=True)
    self_energy = matmul_hi(matmul_hi(tmat, left_in), tmat.T) + matmul_hi(matmul_hi(tmat.T, right_in), tmat)
    dressed = matmul_hi(inverse, self_energy)
    return jnp.diagonal(inverse, axis1=1, axis2=2) + jnp.sum(dressed * jnp.swapaxes(inverse, 1, 2), axis=2)


def operate(values_in, screening):
    padded = jnp.pad(values_in, 1)
    beside = padded[2:, 1:-1, 1:-1] + padded[:-2, 1:-1, 1:-1]
    beside = beside + padded[1:-1, 2:, 1:-1] + padded[1:-1, :-2, 1:-1]
    beside = beside + padded[1:-1, 1:-1, 2:] + padded[1:-1, 1:-1, :-2]
    return (6.0 + screening) * values_in - beside


def reference(layer_inverse, coupling, lead_left, lead_right, quad_weight, energy_slot, plane_of, doping, screening):
    diagonals = lax.map(partial(chain_diagonals, coupling), (layer_inverse, lead_left, lead_right))
    weight = quad_weight[energy_slot]
    layer_density = jnp.sum(weight[:, None, None] * diagonals, axis=0)
    plane_ids = jnp.arange(NX, dtype=jnp.int32)
    onehot = (plane_of[None, :] == plane_ids[:, None]).astype(jnp.float32)
    plane_charge = jnp.dot(onehot, layer_density, precision=exact_mode).reshape(NX, ORB_Y, ORB_Z)
    charge = jnp.repeat(jnp.repeat(plane_charge, NY // ORB_Y, axis=1), NZ // ORB_Z, axis=2)
    source = charge - doping
    potential = jnp.zeros_like(source)
    residual, direction = source, source
    norm_now = jnp.sum(residual * residual)
    for iteration in range(CG_ITERS):
        applied = operate(direction, screening)
        step_size = norm_now / jnp.sum(direction * applied)
        potential = potential + step_size * direction
        residual = residual - step_size * applied
        norm_next = jnp.sum(residual * residual)
        direction = residual + (norm_next / norm_now) * direction
        norm_now = norm_next
    return layer_density, potential, residual
```

```python
import functools

import jax
import jax.numpy as jnp
from jax import lax
from jax.experimental import pallas as pl
from jax.experimental.pallas import tpu as pltpu
from jax.sharding import Mesh
from jax.sharding import PartitionSpec as P

AXES = ("energy_0", "energy_1", "energy_2", "layer_0", "layer_1")
LAYER = ("layer_0", "layer_1")
ENERGY = ("energy_0", "energy_1", "energy_2")
ORB = 16
CG_ITERS = 3
SHIFT = 7.0
PIECES = 2
MESH = pl.DeviceIdType.MESH
HI = lax.Precision.HIGHEST
F32 = jnp.float32
BF16 = jnp.bfloat16


def parts_of(x, count):
    parts = []
    for _ in range(count):
        part = x.astype(BF16)
        parts.append(part)
        x = x - part.astype(F32)
    return parts


def mm(left, right):
    total = None
    most = max(len(left), len(right))
    for i, a in enumerate(left):
        for j, b in enumerate(right):
            if i + j < most:
                term = jnp.dot(a, b, preferred_element_type=F32)
                total = term if total is None else total + term
    return total


def kernel(
    sizes,
    inv_hbm, t_ref, lead_l, lead_r, qw_ref, slot_ref, plane_ref, dop_hbm, scr_hbm,
    dens_out, pot_out, res_out,
    inv, tb, ttb, s_l, s_r, k_l, k_r, acc, e_l, e_r, out_l, out_r,
    dopx, scrx, u1, u2, u3, part, zbuf, pbuf, psrc, mom, zmom, pmom, msrc,
    inv_sem, own_sem, halo_send, halo_recv, relay_send, relay_recv,
    zs, zr, ps, pr, mzs, mzr, mps, mpr,
):
    ny, nxl, nz, nxh, nc = sizes
    y, xl, z, xh, c = [lax.axis_index(a) for a in AXES]
    n_layer = nxh * nc
    n_plane = ny * nxl * n_layer
    n_energy = ny * nxl * nz
    layer = xh * nc + c
    energy = (y * nxl + xl) * nz + z
    slab = energy * n_layer + layer
    n_slabs = n_energy * n_layer
    here = (y * nxl + xl) * n_layer + layer
    count, size, _ = inv_hbm.shape
    planes = dop_hbm.shape[0]

    def plane_dev(index):
        group, lay = lax.div(index, n_layer), lax.rem(index, n_layer)
        return (lax.div(group, nxl), lax.rem(group, nxl), z, lax.div(lay, nc), lax.rem(lay, nc))

    def z_dev(index):
        return (y, xl, index, xh, c)

    def slab_dev(index):
        en, lay = lax.div(index, n_layer), lax.rem(index, n_layer)
        group, zz = lax.div(en, nz), lax.rem(en, nz)
        return (lax.div(group, nxl), lax.rem(group, nxl), zz, lax.div(lay, nc), lax.rem(lay, nc))

    barrier = pltpu.get_barrier_semaphore()
    extra_up = jnp.logical_and(layer == n_layer - 1, energy < n_energy - 1)
    extra_down = jnp.logical_and(layer == 0, energy > 0)
    for k in range(1, nz):
        pl.semaphore_signal(barrier, inc=1, device_id=z_dev(lax.rem(z + k, nz)), device_id_type=MESH)
    for k in range(1, n_plane):
        pl.semaphore_signal(barrier, inc=1, device_id=plane_dev(lax.rem(here + k, n_plane)), device_id_type=MESH)

    @pl.when(extra_up)
    def _():
        pl.semaphore_signal(barrier, inc=1, device_id=slab_dev(slab + 1), device_id_type=MESH)

    @pl.when(extra_down)
    def _():
        pl.semaphore_signal(barrier, inc=1, device_id=slab_dev(slab - 1), device_id_type=MESH)

    loads = []
    for i in range(count // 2):
        for l in (i, count - 1 - i):
            loads.append(pltpu.make_async_copy(inv_hbm.at[l], inv.at[l], inv_sem.at[l]))
    own = [
        pltpu.make_async_copy(dop_hbm, dopx.at[pl.ds(3, planes)], own_sem.at[0]),
        pltpu.make_async_copy(scr_hbm, scrx.at[pl.ds(2, planes)], own_sem.at[1]),
    ]
    for copy in loads + own:
        copy.start()

    t = t_ref[...]
    for n, (piece, across) in enumerate(zip(parts_of(t, PIECES), parts_of(t.T, PIECES))):
        tb[n] = piece
        ttb[n] = across

    rows = lax.broadcasted_iota(jnp.int32, (size, size), 0)
    cols = lax.broadcasted_iota(jnp.int32, (size, size), 1)

    def diagonal(mat):
        return jnp.sum(jnp.where(rows == cols, mat, 0.0), axis=0, keepdims=True)

    def propagators(l, left):
        d = parts_of(inv[l], PIECES)
        a, b = (tb, ttb) if left else (ttb, tb)
        a, b = [a[n] for n in range(PIECES)], [b[n] for n in range(PIECES)]
        return mm(d, a), mm(b, d)

    def first(left):
        l = 0 if left else count - 1
        s, k = (s_l, k_l) if left else (s_r, k_r)
        _, pt = propagators(l, left)
        s[...] = inv[l]
        k[l] = pt
        acc[l : l + 1, :] = jnp.zeros((1, size), F32)

    def step(i, left):
        l = i if left else count - 1 - i
        before = i - 1 if left else count - i
        s, k = (s_l, k_l) if left else (s_r, k_r)
        p, pt = propagators(l, left)
        ptb = parts_of(pt, PIECES)
        y_mat = mm(parts_of(s[...], PIECES), ptb)
        k[l] = mm(parts_of(k[before], PIECES), ptb)
        moved = mm(parts_of(p, PIECES), parts_of(y_mat, PIECES))
        new = inv[l] + moved
        s[...] = new
        return l, diagonal(moved)

    loads[0].wait()
    loads[1].wait()
    first(True)
    first(False)
    for copy in loads[2:]:
        copy.wait()
    for i in range(count):
        acc[i : i + 1, :] = diagonal(inv[i])

    def both(i, carry):
        for left in (True, False):
            l, row = step(i, left)
            acc[pl.ds(l, 1), :] = acc[pl.ds(l, 1), :] + row
        return carry

    lax.fori_loop(1, count, both, 0)

    more = jnp.where(extra_up, 1, 0) + jnp.where(extra_down, 1, 0)
    pl.semaphore_wait(barrier, nz - 1 + n_plane - 1 + more)

    def halo_up():
        dev = slab_dev(slab + 1)
        return [
            pltpu.make_async_remote_copy(
                dop_hbm.at[pl.ds(planes - 3, 3)], dopx.at[pl.ds(0, 3)],
                halo_send.at[0], halo_recv.at[0], device_id=dev, device_id_type=MESH),
            pltpu.make_async_remote_copy(
                scr_hbm.at[pl.ds(planes - 2, 2)], scrx.at[pl.ds(0, 2)],
                halo_send.at[1], halo_recv.at[1], device_id=dev, device_id_type=MESH),
        ]

    def halo_down():
        dev = slab_dev(slab - 1)
        return [
            pltpu.make_async_remote_copy(
                dop_hbm.at[pl.ds(0, 3)], dopx.at[pl.ds(planes + 3, 3)],
                halo_send.at[2], halo_recv.at[2], device_id=dev, device_id_type=MESH),
            pltpu.make_async_remote_copy(
                scr_hbm.at[pl.ds(0, 2)], scrx.at[pl.ds(planes + 2, 2)],
                halo_send.at[3], halo_recv.at[3], device_id=dev, device_id_type=MESH),
        ]

    has_up = slab < n_slabs - 1
    has_down = slab > 0

    @pl.when(has_up)
    def _():
        for copy in halo_up():
            copy.start()

    @pl.when(has_down)
    def _():
        for copy in halo_down():
            copy.start()

    def relay(left):
        out, e = (out_l, e_l) if left else (out_r, e_r)
        n = 0 if left else 1
        to = layer + 1 if left else layer - 1
        dev = plane_dev((y * nxl + xl) * n_layer + to)
        return pltpu.make_async_remote_copy(
            out, e, relay_send.at[n], relay_recv.at[n], device_id=dev, device_id_type=MESH
        )

    def enter(left):
        s, k, e, out = (s_l, k_l, e_l, out_l) if left else (s_r, k_r, e_r, out_r)
        lead = lead_l if left else lead_r
        at_edge = layer == (0 if left else n_layer - 1)
        at_end = layer == (n_layer - 1 if left else 0)

        @pl.when(at_edge)
        def _():
            e[...] = lead[...]

        @pl.when(jnp.logical_not(at_edge))
        def _():
            relay(left).wait_recv()

        eb = parts_of(e[...], PIECES)
        last = count - 1 if left else 0
        k_last = k[last]
        g = mm(eb, parts_of(k_last, PIECES))
        acc[last : last + 1, :] = acc[last : last + 1, :] + jnp.sum(g * k_last, axis=0, keepdims=True)

        @pl.when(jnp.logical_not(at_end))
        def _():
            out[...] = s[...] + mm(parts_of(k_last.T, PIECES), parts_of(g, PIECES))
            relay(left).start()

        for i in range(1, count):
            l = count - 1 - i if left else i
            k_here = k[l]
            g = mm(eb, parts_of(k_here, PIECES))
            acc[l : l + 1, :] = acc[l : l + 1, :] + jnp.sum(g * k_here, axis=0, keepdims=True)

    @pl.when(layer < n_layer // 2)
    def _():
        enter(True)
        enter(False)

    @pl.when(layer >= n_layer // 2)
    def _():
        enter(False)
        enter(True)

    slots = lax.broadcasted_iota(jnp.int32, qw_ref.shape, 1)
    weight = jnp.sum(jnp.where(slots == slot_ref[0], qw_ref[...], 0.0), axis=1, keepdims=True)
    part[...] = weight * acc[...]

    def z_copies(src, buf, send, recv):
        done = []
        for k in range(1, nz):
            to = lax.rem(z + k, nz)
            done.append(pltpu.make_async_remote_copy(
                src, buf.at[z], send.at[to], recv.at[z], device_id=z_dev(to), device_id_type=MESH))
        return done

    def z_arrivals(src, buf, send, recv):
        done = []
        for k in range(1, nz):
            source = lax.rem(z + k, nz)
            done.append(pltpu.make_async_remote_copy(
                src, buf.at[source], send.at[source], recv.at[source], device_id=z_dev(source), device_id_type=MESH))
        return done

    def p_copies(src, buf, send, recv):
        done = []
        for k in range(1, n_plane):
            to = lax.rem(here + k, n_plane)
            done.append(pltpu.make_async_remote_copy(
                src, buf.at[here], send.at[to], recv.at[here], device_id=plane_dev(to), device_id_type=MESH))
        return done

    def p_arrivals(src, buf, send, recv):
        done = []
        for k in range(1, n_plane):
            source = lax.rem(here + k, n_plane)
            done.append(pltpu.make_async_remote_copy(
                src, buf.at[source], send.at[source], recv.at[source], device_id=plane_dev(source), device_id_type=MESH))
        return done

    def exchange(copies, arrivals, src, buf, mine, send, recv):
        for copy in copies(src, buf, send, recv):
            copy.start()
        buf[mine] = src[...]
        for copy in arrivals(src, buf, send, recv):
            copy.wait_recv()

    exchange(z_copies, z_arrivals, part, zbuf, z, zs, zr)
    total = zbuf[0]
    for k in range(1, nz):
        total = total + zbuf[k]
    psrc[...] = total
    exchange(p_copies, p_arrivals, psrc, pbuf, here, ps, pr)
    gathered = []
    for lay in range(n_layer):
        total = pbuf[lay]
        for k in range(1, ny * nxl):
            total = total + pbuf[k * n_layer + lay]
        gathered.append(total)
    dens = jnp.concatenate(gathered, axis=0)
    mine = gathered[0]
    for lay in range(1, n_layer):
        mine = jnp.where(layer == lay, gathered[lay], mine)
    dens_out[...] = mine

    for copy in own:
        copy.wait()

    @pl.when(has_down)
    def _():
        for copy in halo_up():
            copy.wait_recv()

    @pl.when(has_up)
    def _():
        for copy in halo_down():
            copy.wait_recv()

    @pl.when(jnp.logical_not(has_down))
    def _():
        dopx[0:3] = jnp.zeros((3, *dopx.shape[1:]), F32)
        scrx[0:2] = jnp.zeros((2, *scrx.shape[1:]), F32)

    @pl.when(jnp.logical_not(has_up))
    def _():
        dopx[planes + 3 : planes + 6] = jnp.zeros((3, *dopx.shape[1:]), F32)
        scrx[planes + 2 : planes + 4] = jnp.zeros((2, *scrx.shape[1:]), F32)

    low = slab * planes - 3
    n_near = planes + 6
    near = 16
    ids = low + lax.broadcasted_iota(jnp.int32, (near, plane_ref.shape[1]), 0)
    onehot = jnp.where(plane_ref[...] == ids, 1.0, 0.0)
    pc = jnp.dot(onehot, dens, precision=HI, preferred_element_type=F32)
    n_side = dop_hbm.shape[2]
    cell = n_side // ORB
    spread_m = lax.broadcasted_iota(jnp.int32, (size, n_side), 0)
    spread_z = lax.broadcasted_iota(jnp.int32, (size, n_side), 1)
    spread = jnp.where(lax.rem(spread_m, ORB) == lax.div(spread_z, cell), 1.0, 0.0)
    row_j = lax.broadcasted_iota(jnp.int32, (ORB, size), 0)
    row_m = lax.broadcasted_iota(jnp.int32, (ORB, size), 1)
    own_row = row_j == lax.div(row_m, ORB)
    tall = jnp.concatenate([jnp.where(own_row, pc[q : q + 1, :], 0.0) for q in range(n_near)], axis=0)
    wide = jnp.dot(tall, spread, precision=HI, preferred_element_type=F32)
    n_y = dop_hbm.shape[1]
    for q in range(n_near):
        for j in range(ORB):
            row = wide[q * ORB + j : q * ORB + j + 1, :]
            where = pl.ds(j * (n_y // ORB), n_y // ORB)
            dopx[q, where, :] = row - dopx[q, where, :]

    at_y = lax.broadcasted_iota(jnp.int32, (n_y, n_side), 0)
    at_z = lax.broadcasted_iota(jnp.int32, (n_y, n_side), 1)

    def applied(src, dst, trim):
        n_dst = n_near - 2 * trim
        for q in range(n_dst):
            mid = src[q + 1]
            beside = src[q] + src[q + 2]
            beside = beside + jnp.where(at_y == 0, 0.0, pltpu.roll(mid, 1, 0))
            beside = beside + jnp.where(at_y == n_y - 1, 0.0, pltpu.roll(mid, n_y - 1, 0))
            beside = beside + jnp.where(at_z == 0, 0.0, pltpu.roll(mid, 1, 1))
            beside = beside + jnp.where(at_z == n_side - 1, 0.0, pltpu.roll(mid, n_side - 1, 1))
            value = (scrx[q + trim - 1] + (6.0 - SHIFT)) * mid - beside
            if q < 3 - trim:
                value = jnp.where(has_down, value, 0.0)
            if q >= 3 - trim + planes:
                value = jnp.where(has_up, value, 0.0)
            dst[q] = value

    applied(dopx, u1, 1)
    applied(u1, u2, 2)
    applied(u2, u3, 3)

    def inner(a, a0, b, b0):
        total = None
        for q in range(planes):
            term = a[a0 + q] * b[b0 + q]
            total = term if total is None else total + term
        return jnp.sum(jnp.sum(total, axis=0, keepdims=True), axis=1, keepdims=True)

    sums = [
        inner(dopx, 3, dopx, 3), inner(dopx, 3, u1, 2), inner(u1, 2, u1, 2),
        inner(u1, 2, u2, 1), inner(u2, 1, u2, 1), inner(u2, 1, u3, 0),
    ]
    lane = lax.broadcasted_iota(jnp.int32, (1, 128), 1)
    row = jnp.zeros((1, 128), F32)
    for k, value in enumerate(sums):
        row = jnp.where(lane == k, value, row)
    mom[...] = row
    exchange(z_copies, z_arrivals, mom, zmom, z, mzs, mzr)
    total = zmom[0]
    for k in range(1, nz):
        total = total + zmom[k]
    msrc[...] = total
    exchange(p_copies, p_arrivals, msrc, pmom, here, mps, mpr)
    total = pmom[0]
    for k in range(1, n_plane):
        total = total + pmom[k]
    moment = [total[:, k : k + 1] for k in range(6)]

    def product(a, b):
        value = None
        for i, p in enumerate(a):
            for j, q in enumerate(b):
                term = p * q * moment[i + j]
                value = term if value is None else value + term
        return value

    def times_a(a):
        shifted = [None, *a]
        kept = [SHIFT * v for v in a] + [None]
        return [w if v is None else v if w is None else v + w for v, w in zip(shifted, kept)]

    def plus(a, factor, b):
        longest = max(len(a), len(b))
        result = []
        for i in range(longest):
            if i >= len(b):
                result.append(a[i])
            elif i >= len(a):
                result.append(factor * b[i])
            else:
                result.append(a[i] + factor * b[i])
        return result

    one = jnp.ones((1, 1), F32)
    residual, direction, potential = [one], [one], []
    norm = moment[0]
    for iteration in range(CG_ITERS):
        a_dir = times_a(direction)
        step_size = norm / product(direction, a_dir)
        potential = plus(potential, step_size, direction)
        residual = plus(residual, -step_size, a_dir)
        if iteration + 1 < CG_ITERS:
            new = product(residual, residual)
            direction = plus(residual, new / norm, direction)
            norm = new

    for q in range(planes):
        v = [dopx[3 + q], u1[2 + q], u2[1 + q], u3[q]]
        x = potential[0] * v[0]
        for k in range(1, CG_ITERS):
            x = x + potential[k] * v[k]
        pot_out[q] = x
        r = residual[0] * v[0]
        for k in range(1, CG_ITERS + 1):
            r = r + residual[k] * v[k]
        res_out[q] = r

    for copy in z_copies(part, zbuf, zs, zr) + z_copies(mom, zmom, mzs, mzr):
        copy.wait_send()
    for copy in p_copies(psrc, pbuf, ps, pr) + p_copies(msrc, pmom, mps, mpr):
        copy.wait_send()

    @pl.when(layer < n_layer - 1)
    def _():
        relay(True).wait_send()

    @pl.when(layer > 0)
    def _():
        relay(False).wait_send()

    @pl.when(has_up)
    def _():
        for copy in halo_up():
            copy.wait_send()

    @pl.when(has_down)
    def _():
        for copy in halo_down():
            copy.wait_send()


def body(
    sizes,
    layer_inverse,
    coupling,
    lead_left,
    lead_right,
    quad_weight,
    energy_slot,
    plane_of,
    doping,
    screening,
):
    ny, nxl, nz, nxh, nc = sizes
    _, count, size, _ = layer_inverse.shape
    planes, n_y, n_z = doping.shape
    n_plane = ny * nxl * nxh * nc
    vmem = pl.BlockSpec(memory_space=pltpu.VMEM)
    hbm = pl.BlockSpec(memory_space=pl.ANY)
    smem = pl.BlockSpec(memory_space=pltpu.SMEM)
    square = pltpu.VMEM((size, size), F32)
    squares = pltpu.VMEM((count, size, size), F32)
    dma = pltpu.SemaphoreType.DMA
    rows = pltpu.VMEM((count, size), F32)
    return pl.pallas_call(
        functools.partial(kernel, sizes),
        out_shape=(
            jax.ShapeDtypeStruct((count, size), F32),
            jax.ShapeDtypeStruct(doping.shape, F32),
            jax.ShapeDtypeStruct(doping.shape, F32),
        ),
        in_specs=[hbm, vmem, vmem, vmem, vmem, smem, vmem, hbm, hbm],
        out_specs=(vmem, vmem, vmem),
        scratch_shapes=[
            squares,
            pltpu.VMEM((PIECES, size, size), BF16),
            pltpu.VMEM((PIECES, size, size), BF16),
            square, square, squares, squares, rows, square, square, square, square,
            pltpu.VMEM((planes + 6, n_y, n_z), F32),
            pltpu.VMEM((planes + 4, n_y, n_z), F32),
            pltpu.VMEM((planes + 4, n_y, n_z), F32),
            pltpu.VMEM((planes + 2, n_y, n_z), F32),
            pltpu.VMEM((planes, n_y, n_z), F32),
            rows,
            pltpu.VMEM((nz, count, size), F32),
            pltpu.VMEM((n_plane, count, size), F32),
            rows,
            pltpu.VMEM((1, 128), F32),
            pltpu.VMEM((nz, 1, 128), F32),
            pltpu.VMEM((n_plane, 1, 128), F32),
            pltpu.VMEM((1, 128), F32),
            dma((count,)), dma((2,)), dma((4,)), dma((4,)), dma((2,)), dma((2,)),
            dma((nz,)), dma((nz,)), dma((n_plane,)), dma((n_plane,)),
            dma((nz,)), dma((nz,)), dma((n_plane,)), dma((n_plane,)),
        ],
        compiler_params=pltpu.CompilerParams(
            collective_id=0, has_side_effects=True, vmem_limit_bytes=48 * 1024 * 1024
        ),
    )(
        layer_inverse[0],
        coupling,
        lead_left[0],
        lead_right[0],
        quad_weight[None],
        energy_slot,
        plane_of[None],
        doping,
        screening,
    )


def sharded(split):
    energy_layer = (*ENERGY, *LAYER)
    in_specs = (
        P(ENERGY, LAYER, None, None),
        P(),
        P(ENERGY, None, None),
        P(ENERGY, None, None),
        P(),
        P(ENERGY),
        P(),
        P(energy_layer, None, None),
        P(energy_layer, None, None),
    )
    out_specs = (P(LAYER, None), P(energy_layer, None, None), P(energy_layer, None, None))
    sizes = tuple(split.shape[a] for a in AXES)
    return jax.shard_map(
        functools.partial(body, sizes), mesh=split, in_specs=in_specs, out_specs=out_specs, check_vma=False
    )


def solution(mesh):
    return sharded(Mesh(mesh.devices.reshape(4, 2, 8, 2, 2), AXES))
```

```python
import functools

import jax
import jax.numpy as jnp
from jax import lax
from jax.experimental import pallas as pl
from jax.experimental.pallas import tpu as pltpu
from jax.sharding import Mesh
from jax.sharding import PartitionSpec as P

AXES = ("energy_0", "energy_1", "energy_2", "layer_0", "layer_1")
LAYER = ("layer_0", "layer_1")
ENERGY = ("energy_0", "energy_1", "energy_2")
ORB = 16
CG_ITERS = 3
SHIFT = 7.0
VMEM = 48 * 1024 * 1024
PROP = (2, 2)
PULL = (2, 2)
CARRY = (2, 2)
MOVE = (2, 2)
ENTER = (1, 1)
LEAVE = (1, 1)
MESH = pl.DeviceIdType.MESH
HI = lax.Precision.HIGHEST
F32 = jnp.float32
BF16 = jnp.bfloat16


def parts_of(x, count):
    parts = []
    for _ in range(count):
        part = x.astype(BF16)
        parts.append(part)
        x = x - part.astype(F32)
    return parts


def mm(left, right):
    total = None
    most = max(len(left), len(right))
    for i, a in enumerate(left):
        for j, b in enumerate(right):
            if i + j < most:
                term = jnp.dot(a, b, preferred_element_type=F32)
                total = term if total is None else total + term
    return total


def kernel(
    sizes,
    inv_hbm, t_hbm, lead_l, lead_r, qw_hbm, slot_hbm, plane_hbm, dop_hbm, scr_hbm,
    dens_out, pot_out, res_out,
    inv, t_ref, tt, p_b, pt_b, s_ref, k_ref, acc, e_ref, wire_in, wire_out, qw_ref, slot_ref, plane_ref,
    dopx, scrx, u1, u2, u3, part, zbuf, pbuf, psrc, mom, zmom, pmom, msrc,
    inv_sem, own_sem, halo_send, halo_recv, relay_send, relay_recv,
    zs, zr, ps, pr, mzs, mzr, mps, mpr,
):
    ny, nxl, nz, nxh, nc = sizes
    y, xl, z, xh, c = [lax.axis_index(a) for a in AXES]
    n_layer = nxh * nc
    n_plane = ny * nxl * n_layer
    n_energy = ny * nxl * nz
    layer = xh * nc + c
    energy = (y * nxl + xl) * nz + z
    slab = energy * n_layer + layer
    n_slabs = n_energy * n_layer
    here = (y * nxl + xl) * n_layer + layer
    count, size, _ = inv_hbm.shape
    planes = dop_hbm.shape[0]

    def plane_dev(index):
        group, lay = lax.div(index, n_layer), lax.rem(index, n_layer)
        return (lax.div(group, nxl), lax.rem(group, nxl), z, lax.div(lay, nc), lax.rem(lay, nc))

    def z_dev(index):
        return (y, xl, index, xh, c)

    def slab_dev(index):
        en, lay = lax.div(index, n_layer), lax.rem(index, n_layer)
        group, zz = lax.div(en, nz), lax.rem(en, nz)
        return (lax.div(group, nxl), lax.rem(group, nxl), zz, lax.div(lay, nc), lax.rem(lay, nc))

    barrier = pltpu.get_barrier_semaphore()
    extra_up = jnp.logical_and(layer == n_layer - 1, energy < n_energy - 1)
    extra_down = jnp.logical_and(layer == 0, energy > 0)
    for k in range(1, nz):
        pl.semaphore_signal(barrier, inc=1, device_id=z_dev(lax.rem(z + k, nz)), device_id_type=MESH)
    for k in range(1, n_plane):
        pl.semaphore_signal(barrier, inc=1, device_id=plane_dev(lax.rem(here + k, n_plane)), device_id_type=MESH)

    @pl.when(extra_up)
    def _():
        pl.semaphore_signal(barrier, inc=1, device_id=slab_dev(slab + 1), device_id_type=MESH)

    @pl.when(extra_down)
    def _():
        pl.semaphore_signal(barrier, inc=1, device_id=slab_dev(slab - 1), device_id_type=MESH)

    first = jnp.where(layer >= n_layer // 2, 1, 0)

    def layer_at(q, i):
        return q * (count - 1) + (1 - 2 * q) * i

    t_load = pltpu.make_async_copy(t_hbm, t_ref, own_sem.at[2])
    t_load.start()
    for i in range(count):
        l = layer_at(first, i)
        pltpu.make_async_copy(inv_hbm.at[l], inv.at[l], inv_sem.at[l]).start()
    lead_loads = [
        pltpu.make_async_copy(lead_l, e_ref.at[0], own_sem.at[3]),
        pltpu.make_async_copy(lead_r, e_ref.at[1], own_sem.at[4]),
    ]
    edges = [layer == 0, layer == n_layer - 1]
    for edge, copy in zip(edges, lead_loads):
        pl.when(edge)(copy.start)
    own = [
        pltpu.make_async_copy(dop_hbm, dopx.at[pl.ds(3, planes)], own_sem.at[0]),
        pltpu.make_async_copy(scr_hbm, scrx.at[pl.ds(2, planes)], own_sem.at[1]),
        pltpu.make_async_copy(qw_hbm, qw_ref, own_sem.at[5]),
        pltpu.make_async_copy(slot_hbm, slot_ref, own_sem.at[6]),
        pltpu.make_async_copy(plane_hbm, plane_ref, own_sem.at[7]),
    ]
    for copy in own:
        copy.start()

    t_load.wait()
    t = t_ref[...]
    for n, (piece, across) in enumerate(zip(parts_of(t, PROP[1]), parts_of(t.T, PROP[1]))):
        tt[0, n] = piece
        tt[1, n] = across

    rows = lax.broadcasted_iota(jnp.int32, (size, size), 0)
    cols = lax.broadcasted_iota(jnp.int32, (size, size), 1)

    def diagonal(mat):
        return jnp.sum(jnp.where(rows == cols, mat, 0.0), axis=0, keepdims=True)

    def propagator(q, i):
        d = parts_of(inv[layer_at(q, i)], PROP[0])
        a = [tt[q, n] for n in range(PROP[1])]
        b = [tt[1 - q, n] for n in range(PROP[1])]
        return mm(d, a), mm(b, d)

    def keep(slot, p, pt):
        for n, piece in enumerate(parts_of(p, MOVE[0])):
            p_b[slot, n] = piece
        for n, piece in enumerate(parts_of(pt, max(PULL[1], CARRY[1]))):
            pt_b[slot, n] = piece

    def begin(q):
        l = layer_at(q, 0)
        s_ref[q] = inv[l]
        _, pt = propagator(q, 0)
        k_ref[q, l] = pt
        keep(1, *propagator(q, 1))

    def step(q, i):
        l, before = layer_at(q, i), layer_at(q, i - 1)
        now, later = lax.rem(i, 2), lax.rem(i + 1, 2)
        pt = [pt_b[now, n] for n in range(max(PULL[1], CARRY[1]))]
        p = [p_b[now, n] for n in range(MOVE[0])]
        y_mat = mm(parts_of(s_ref[q], PULL[0]), pt[: PULL[1]])
        k_new = mm(parts_of(k_ref[q, before], CARRY[0]), pt[: CARRY[1]])
        p_next, pt_next = propagator(q, jnp.minimum(i + 1, count - 1))
        moved = mm(p, parts_of(y_mat, MOVE[1]))
        keep(later, p_next, pt_next)
        k_ref[q, l] = k_new
        s_ref[q] = inv[l] + moved
        acc[pl.ds(l, 1), :] = acc[pl.ds(l, 1), :] + diagonal(moved)

    def halo_up():
        dev = slab_dev(slab + 1)
        return [
            pltpu.make_async_remote_copy(
                dop_hbm.at[pl.ds(planes - 3, 3)], dopx.at[pl.ds(0, 3)],
                halo_send.at[0], halo_recv.at[0], device_id=dev, device_id_type=MESH),
            pltpu.make_async_remote_copy(
                scr_hbm.at[pl.ds(planes - 2, 2)], scrx.at[pl.ds(0, 2)],
                halo_send.at[1], halo_recv.at[1], device_id=dev, device_id_type=MESH),
        ]

    def halo_down():
        dev = slab_dev(slab - 1)
        return [
            pltpu.make_async_remote_copy(
                dop_hbm.at[pl.ds(0, 3)], dopx.at[pl.ds(planes + 3, 3)],
                halo_send.at[2], halo_recv.at[2], device_id=dev, device_id_type=MESH),
            pltpu.make_async_remote_copy(
                scr_hbm.at[pl.ds(0, 2)], scrx.at[pl.ds(planes + 2, 2)],
                halo_send.at[3], halo_recv.at[3], device_id=dev, device_id_type=MESH),
        ]

    has_up = slab < n_slabs - 1
    has_down = slab > 0

    half = size // 2
    r_half = lax.broadcasted_iota(jnp.int32, (half, half), 0)
    c_half = lax.broadcasted_iota(jnp.int32, (half, half), 1)

    def pack(q, mat):
        one, two = mat[:half, :half], mat[half:, half:]
        wire_out[q, 0:half] = mat[:half, half:]
        wire_out[q, half:size] = jnp.where(r_half <= c_half, one, two)
        line = jnp.sum(jnp.where(r_half == c_half, two, 0.0), axis=0, keepdims=True)
        wire_out[q, size : size + 8] = jnp.broadcast_to(line, (8, half))

    def unpack(q):
        side, both = wire_in[q, 0:half], wire_in[q, half:size]
        over = both.T
        line = wire_in[q, size : size + 1]
        e_ref[q, 0:half, half:size] = side
        e_ref[q, half:size, 0:half] = side.T
        e_ref[q, 0:half, 0:half] = jnp.where(r_half <= c_half, both, over)
        two = jnp.where(r_half > c_half, both, over)
        e_ref[q, half:size, half:size] = jnp.where(r_half == c_half, line, two)

    def relay(q):
        dev = plane_dev(here + 1 - 2 * q)
        return pltpu.make_async_remote_copy(
            wire_out.at[q], wire_in.at[q], relay_send.at[q], relay_recv.at[q], device_id=dev, device_id_type=MESH
        )

    def row_of(q, eb, l):
        k_here = k_ref[q, l]
        g = mm(eb, parts_of(k_here, ENTER[1]))
        return k_here, g, jnp.sum(g * k_here, axis=0, keepdims=True)

    def add_row(l, row):
        acc[pl.ds(l, 1), :] = acc[pl.ds(l, 1), :] + row

    def pass_on(q):
        at_end = layer == (1 - q) * (n_layer - 1)
        l = layer_at(q, count - 1)
        k_last, g, row = row_of(q, parts_of(e_ref[q], ENTER[0]), l)

        @pl.when(jnp.logical_not(at_end))
        def _():
            pack(q, s_ref[q] + mm(parts_of(k_last.T, LEAVE[0]), parts_of(g, LEAVE[1])))
            relay(q).start()

        add_row(l, row)

    def rest(q):
        eb = parts_of(e_ref[q], ENTER[0])
        found = [row_of(q, eb, layer_at(q, i))[2] for i in range(count - 1)]
        for i, row in enumerate(found):
            add_row(layer_at(q, i), row)

    second = 1 - first
    for i in range(2):
        l = layer_at(first, i)
        pltpu.make_async_copy(inv_hbm.at[l], inv.at[l], inv_sem.at[l]).wait()
    begin(first)
    for i in range(2, count):
        l = layer_at(first, i)
        pltpu.make_async_copy(inv_hbm.at[l], inv.at[l], inv_sem.at[l]).wait()
    for i in range(count):
        acc[i : i + 1, :] = diagonal(inv[i])

    def chain_first(i, carry):
        step(first, i)
        return carry

    lax.fori_loop(1, count, chain_first, 0)

    more = jnp.where(extra_up, 1, 0) + jnp.where(extra_down, 1, 0)
    pl.semaphore_wait(barrier, nz - 1 + n_plane - 1 + more)
    for edge, copy in zip(edges, lead_loads):
        pl.when(edge)(copy.wait)
    outer = jnp.logical_or(*edges)
    inner_seg = jnp.logical_not(outer)

    @pl.when(inner_seg)
    def _():
        begin(second)
        relay(first).wait_recv()
        unpack(first)

    pass_on(first)

    @pl.when(has_up)
    def _():
        for copy in halo_up():
            copy.start()

    @pl.when(has_down)
    def _():
        for copy in halo_down():
            copy.start()

    @pl.when(outer)
    def _():
        begin(second)

    def chain_second(i, carry):
        step(second, i)
        return carry

    lax.fori_loop(1, count, chain_second, 0)

    @pl.when(outer)
    def _():
        rest(first)

    relay(second).wait_recv()
    unpack(second)
    pass_on(second)

    @pl.when(inner_seg)
    def _():
        rest(first)

    rest(second)

    for copy in own:
        copy.wait()
    slots = lax.broadcasted_iota(jnp.int32, qw_ref.shape, 1)
    weight = jnp.sum(jnp.where(slots == slot_ref[...], qw_ref[...], 0.0), axis=1, keepdims=True)
    part[...] = weight * acc[...]

    def z_copies(src, buf, send, recv):
        done = []
        for k in range(1, nz):
            to = lax.rem(z + k, nz)
            done.append(pltpu.make_async_remote_copy(
                src, buf.at[z], send.at[to], recv.at[z], device_id=z_dev(to), device_id_type=MESH))
        return done

    def z_arrivals(src, buf, send, recv):
        done = []
        for k in range(1, nz):
            source = lax.rem(z + k, nz)
            done.append(pltpu.make_async_remote_copy(
                src, buf.at[source], send.at[source], recv.at[source], device_id=z_dev(source), device_id_type=MESH))
        return done

    def p_copies(src, buf, send, recv):
        done = []
        for k in range(1, n_plane):
            to = lax.rem(here + k, n_plane)
            done.append(pltpu.make_async_remote_copy(
                src, buf.at[here], send.at[to], recv.at[here], device_id=plane_dev(to), device_id_type=MESH))
        return done

    def p_arrivals(src, buf, send, recv):
        done = []
        for k in range(1, n_plane):
            source = lax.rem(here + k, n_plane)
            done.append(pltpu.make_async_remote_copy(
                src, buf.at[source], send.at[source], recv.at[source], device_id=plane_dev(source), device_id_type=MESH))
        return done

    def exchange(copies, arrivals, src, buf, mine, send, recv):
        for copy in copies(src, buf, send, recv):
            copy.start()
        buf[mine] = src[...]
        for copy in arrivals(src, buf, send, recv):
            copy.wait_recv()

    exchange(z_copies, z_arrivals, part, zbuf, z, zs, zr)
    total = zbuf[0]
    for k in range(1, nz):
        total = total + zbuf[k]
    psrc[...] = total
    exchange(p_copies, p_arrivals, psrc, pbuf, here, ps, pr)
    gathered = []
    for lay in range(n_layer):
        total = pbuf[lay]
        for k in range(1, ny * nxl):
            total = total + pbuf[k * n_layer + lay]
        gathered.append(total)
    dens = jnp.concatenate(gathered, axis=0)
    mine = gathered[0]
    for lay in range(1, n_layer):
        mine = jnp.where(layer == lay, gathered[lay], mine)
    dens_out[...] = mine

    @pl.when(has_down)
    def _():
        for copy in halo_up():
            copy.wait_recv()

    @pl.when(has_up)
    def _():
        for copy in halo_down():
            copy.wait_recv()

    @pl.when(jnp.logical_not(has_down))
    def _():
        dopx[0:3] = jnp.zeros((3, *dopx.shape[1:]), F32)
        scrx[0:2] = jnp.zeros((2, *scrx.shape[1:]), F32)

    @pl.when(jnp.logical_not(has_up))
    def _():
        dopx[planes + 3 : planes + 6] = jnp.zeros((3, *dopx.shape[1:]), F32)
        scrx[planes + 2 : planes + 4] = jnp.zeros((2, *scrx.shape[1:]), F32)

    low = slab * planes - 3
    n_near = planes + 6
    near = 16
    ids = low + lax.broadcasted_iota(jnp.int32, (near, plane_ref.shape[1]), 0)
    onehot = jnp.where(plane_ref[...] == ids, 1.0, 0.0)
    pc = jnp.dot(onehot, dens, precision=HI, preferred_element_type=F32)
    n_side = dop_hbm.shape[2]
    cell = n_side // ORB
    spread_m = lax.broadcasted_iota(jnp.int32, (size, n_side), 0)
    spread_z = lax.broadcasted_iota(jnp.int32, (size, n_side), 1)
    spread = jnp.where(lax.rem(spread_m, ORB) == lax.div(spread_z, cell), 1.0, 0.0)
    row_j = lax.broadcasted_iota(jnp.int32, (ORB, size), 0)
    row_m = lax.broadcasted_iota(jnp.int32, (ORB, size), 1)
    own_row = row_j == lax.div(row_m, ORB)
    tall = jnp.concatenate([jnp.where(own_row, pc[q : q + 1, :], 0.0) for q in range(n_near)], axis=0)
    wide = jnp.dot(tall, spread, precision=HI, preferred_element_type=F32)
    n_y = dop_hbm.shape[1]
    for q in range(n_near):
        for j in range(ORB):
            row = wide[q * ORB + j : q * ORB + j + 1, :]
            where = pl.ds(j * (n_y // ORB), n_y // ORB)
            dopx[q, where, :] = row - dopx[q, where, :]

    at_y = lax.broadcasted_iota(jnp.int32, (n_y, n_side), 0)
    at_z = lax.broadcasted_iota(jnp.int32, (n_y, n_side), 1)

    def applied(src, dst, trim):
        n_dst = n_near - 2 * trim
        for q in range(n_dst):
            mid = src[q + 1]
            beside = src[q] + src[q + 2]
            beside = beside + jnp.where(at_y == 0, 0.0, pltpu.roll(mid, 1, 0))
            beside = beside + jnp.where(at_y == n_y - 1, 0.0, pltpu.roll(mid, n_y - 1, 0))
            beside = beside + jnp.where(at_z == 0, 0.0, pltpu.roll(mid, 1, 1))
            beside = beside + jnp.where(at_z == n_side - 1, 0.0, pltpu.roll(mid, n_side - 1, 1))
            value = (scrx[q + trim - 1] + (6.0 - SHIFT)) * mid - beside
            if q < 3 - trim:
                value = jnp.where(has_down, value, 0.0)
            if q >= 3 - trim + planes:
                value = jnp.where(has_up, value, 0.0)
            dst[q] = value

    applied(dopx, u1, 1)
    applied(u1, u2, 2)
    applied(u2, u3, 3)

    def inner(a, a0, b, b0):
        total = None
        for q in range(planes):
            term = a[a0 + q] * b[b0 + q]
            total = term if total is None else total + term
        return jnp.sum(jnp.sum(total, axis=0, keepdims=True), axis=1, keepdims=True)

    sums = [
        inner(dopx, 3, dopx, 3), inner(dopx, 3, u1, 2), inner(u1, 2, u1, 2),
        inner(u1, 2, u2, 1), inner(u2, 1, u2, 1), inner(u2, 1, u3, 0),
    ]
    lane = lax.broadcasted_iota(jnp.int32, (1, 128), 1)
    row = jnp.zeros((1, 128), F32)
    for k, value in enumerate(sums):
        row = jnp.where(lane == k, value, row)
    mom[...] = row
    exchange(z_copies, z_arrivals, mom, zmom, z, mzs, mzr)
    total = zmom[0]
    for k in range(1, nz):
        total = total + zmom[k]
    msrc[...] = total
    exchange(p_copies, p_arrivals, msrc, pmom, here, mps, mpr)
    total = pmom[0]
    for k in range(1, n_plane):
        total = total + pmom[k]
    moment = [total[:, k : k + 1] for k in range(6)]

    def product(a, b):
        value = None
        for i, p in enumerate(a):
            for j, q in enumerate(b):
                term = p * q * moment[i + j]
                value = term if value is None else value + term
        return value

    def times_a(a):
        shifted = [None, *a]
        kept = [SHIFT * v for v in a] + [None]
        return [w if v is None else v if w is None else v + w for v, w in zip(shifted, kept)]

    def plus(a, factor, b):
        longest = max(len(a), len(b))
        result = []
        for i in range(longest):
            if i >= len(b):
                result.append(a[i])
            elif i >= len(a):
                result.append(factor * b[i])
            else:
                result.append(a[i] + factor * b[i])
        return result

    one = jnp.ones((1, 1), F32)
    residual, direction, potential = [one], [one], []
    norm = moment[0]
    for iteration in range(CG_ITERS):
        a_dir = times_a(direction)
        step_size = norm / product(direction, a_dir)
        potential = plus(potential, step_size, direction)
        residual = plus(residual, -step_size, a_dir)
        if iteration + 1 < CG_ITERS:
            new = product(residual, residual)
            direction = plus(residual, new / norm, direction)
            norm = new

    for q in range(planes):
        v = [dopx[3 + q], u1[2 + q], u2[1 + q], u3[q]]
        x = potential[0] * v[0]
        for k in range(1, CG_ITERS):
            x = x + potential[k] * v[k]
        pot_out[q] = x
        r = residual[0] * v[0]
        for k in range(1, CG_ITERS + 1):
            r = r + residual[k] * v[k]
        res_out[q] = r

    for copy in z_copies(part, zbuf, zs, zr) + z_copies(mom, zmom, mzs, mzr):
        copy.wait_send()
    for copy in p_copies(psrc, pbuf, ps, pr) + p_copies(msrc, pmom, mps, mpr):
        copy.wait_send()

    relay(first).wait_send()

    @pl.when(inner_seg)
    def _():
        relay(second).wait_send()

    @pl.when(has_up)
    def _():
        for copy in halo_up():
            copy.wait_send()

    @pl.when(has_down)
    def _():
        for copy in halo_down():
            copy.wait_send()


def body(
    sizes,
    layer_inverse,
    coupling,
    lead_left,
    lead_right,
    quad_weight,
    energy_slot,
    plane_of,
    doping,
    screening,
):
    ny, nxl, nz, nxh, nc = sizes
    _, count, size, _ = layer_inverse.shape
    planes, n_y, n_z = doping.shape
    n_plane = ny * nxl * nxh * nc
    vmem = pl.BlockSpec(memory_space=pltpu.VMEM)
    hbm = pl.BlockSpec(memory_space=pltpu.HBM)
    square = pltpu.VMEM((size, size), F32)
    squares = pltpu.VMEM((count, size, size), F32)
    dma = pltpu.SemaphoreType.DMA
    rows = pltpu.VMEM((count, size), F32)
    operands = (
        layer_inverse[0], coupling, lead_left[0], lead_right[0], quad_weight[None], energy_slot[None], plane_of[None],
        doping, screening,
    )
    return pl.pallas_call(
        functools.partial(kernel, sizes),
        out_shape=(
            jax.ShapeDtypeStruct((count, size), F32),
            jax.ShapeDtypeStruct(doping.shape, F32),
            jax.ShapeDtypeStruct(doping.shape, F32),
        ),
        in_specs=[hbm] * 9,
        out_specs=(vmem, vmem, vmem),
        scratch_shapes=[
            squares,
            square,
            pltpu.VMEM((2, PROP[1], size, size), BF16),
            pltpu.VMEM((2, MOVE[0], size, size), BF16),
            pltpu.VMEM((2, max(PULL[1], CARRY[1]), size, size), BF16),
            pltpu.VMEM((2, size, size), F32),
            pltpu.VMEM((2, count, size, size), F32),
            rows,
            pltpu.VMEM((2, size, size), F32),
            pltpu.VMEM((2, size + 8, size // 2), F32),
            pltpu.VMEM((2, size + 8, size // 2), F32),
            pltpu.VMEM((1, quad_weight.shape[0]), F32),
            pltpu.VMEM((1, 1), jnp.int32),
            pltpu.VMEM((1, plane_of.shape[0]), jnp.int32),
            pltpu.VMEM((planes + 6, n_y, n_z), F32),
            pltpu.VMEM((planes + 4, n_y, n_z), F32),
            pltpu.VMEM((planes + 4, n_y, n_z), F32),
            pltpu.VMEM((planes + 2, n_y, n_z), F32),
            pltpu.VMEM((planes, n_y, n_z), F32),
            rows,
            pltpu.VMEM((nz, count, size), F32),
            pltpu.VMEM((n_plane, count, size), F32),
            rows,
            pltpu.VMEM((1, 128), F32),
            pltpu.VMEM((nz, 1, 128), F32),
            pltpu.VMEM((n_plane, 1, 128), F32),
            pltpu.VMEM((1, 128), F32),
            dma((count,)), dma((8,)), dma((4,)), dma((4,)), dma((2,)), dma((2,)),
            dma((nz,)), dma((nz,)), dma((n_plane,)), dma((n_plane,)),
            dma((nz,)), dma((nz,)), dma((n_plane,)), dma((n_plane,)),
        ],
        compiler_params=pltpu.CompilerParams(
            collective_id=0, has_side_effects=True, vmem_limit_bytes=VMEM
        ),
    )(*[v if v.size == 1 else pltpu.with_memory_space_constraint(v, pltpu.HBM) for v in operands])


def sharded(split):
    energy_layer = (*ENERGY, *LAYER)
    in_specs = (
        P(ENERGY, LAYER, None, None),
        P(),
        P(ENERGY, None, None),
        P(ENERGY, None, None),
        P(),
        P(ENERGY),
        P(),
        P(energy_layer, None, None),
        P(energy_layer, None, None),
    )
    out_specs = (P(LAYER, None), P(energy_layer, None, None), P(energy_layer, None, None))
    sizes = tuple(split.shape[a] for a in AXES)
    return jax.shard_map(
        functools.partial(body, sizes), mesh=split, in_specs=in_specs, out_specs=out_specs, check_vma=False
    )


def solution(mesh):
    return sharded(Mesh(mesh.devices.reshape(4, 2, 8, 2, 2), AXES))
```

```python
import functools

import jax
import jax.numpy as jnp
from jax import lax
from jax.experimental import pallas as pl
from jax.experimental.pallas import tpu as pltpu
from jax.sharding import Mesh
from jax.sharding import PartitionSpec as P

AXES = ("energy_0", "energy_1", "energy_2", "layer_0", "layer_1")
LAYER = ("layer_0", "layer_1")
ENERGY = ("energy_0", "energy_1", "energy_2")
ORB = 16
CG_ITERS = 3
SHIFT = 7.0
VMEM = 48 * 1024 * 1024
PULL = (2, 2)
CARRY = (2, 2)
MOVE = (2, 2)
ENTER = (1, 1)
LEAVE = (1, 1)
EARLY = 1
MEET = 4
MESH = pl.DeviceIdType.MESH
HI = lax.Precision.HIGHEST
F32 = jnp.float32
BF16 = jnp.bfloat16


def parts_of(x, count):
    parts = []
    for _ in range(count):
        part = x.astype(BF16)
        parts.append(part)
        x = x - part.astype(F32)
    return parts


def mm(left, right):
    total = None
    most = max(len(left), len(right))
    for i, a in enumerate(left):
        for j, b in enumerate(right):
            if i + j < most:
                term = jnp.dot(a, b, preferred_element_type=F32)
                total = term if total is None else total + term
    return total


def kernel(
    sizes,
    inv_hbm, t_hbm, lead_l, lead_r, qw_hbm, slot_hbm, plane_hbm, dop_hbm, scr_hbm,
    dens_out, pot_out, res_out,
    inv, t_ref, t_both, t_b, s_ref, k_ref, acc, e_ref, wire_in, wire_out, qw_ref, slot_ref, plane_ref,
    dopx, scrx, u1, u2, u3, part, zbuf, psrc, pbuf, mom, zmom, pmom, msrc,
    inv_sem, own_sem, halo_send, halo_recv, relay_send, relay_recv,
    zs, zr, ps, pr, mzs, mzr, mps, mpr,
):
    ny, nxl, nz, nxh, nc = sizes
    y, xl, z, xh, c = [lax.axis_index(a) for a in AXES]
    n_layer = nxh * nc
    n_plane = ny * nxl * n_layer
    n_energy = ny * nxl * nz
    layer = xh * nc + c
    energy = (y * nxl + xl) * nz + z
    slab = energy * n_layer + layer
    n_slabs = n_energy * n_layer
    here = (y * nxl + xl) * n_layer + layer
    count, size, _ = inv_hbm.shape
    planes = dop_hbm.shape[0]

    def plane_dev(index):
        group, lay = lax.div(index, n_layer), lax.rem(index, n_layer)
        return (lax.div(group, nxl), lax.rem(group, nxl), z, lax.div(lay, nc), lax.rem(lay, nc))

    def z_dev(index):
        return (y, xl, index, xh, c)

    def slab_dev(index):
        en, lay = lax.div(index, n_layer), lax.rem(index, n_layer)
        group, zz = lax.div(en, nz), lax.rem(en, nz)
        return (lax.div(group, nxl), lax.rem(group, nxl), zz, lax.div(lay, nc), lax.rem(lay, nc))

    first = jnp.where(layer >= n_layer // 2, 1, 0)

    def layer_at(q, i):
        return q * (count - 1) + (1 - 2 * q) * i

    t_load = pltpu.make_async_copy(t_hbm, t_ref, own_sem.at[2])
    t_load.start()
    for i in range(count):
        l = layer_at(first, i)
        pltpu.make_async_copy(inv_hbm.at[l], inv.at[l], inv_sem.at[l]).start()
    lead_loads = [
        pltpu.make_async_copy(lead_l, e_ref.at[0], own_sem.at[3]),
        pltpu.make_async_copy(lead_r, e_ref.at[1], own_sem.at[4]),
    ]
    edges = [layer == 0, layer == n_layer - 1]
    for edge, copy in zip(edges, lead_loads):
        pl.when(edge)(copy.start)
    own = [
        pltpu.make_async_copy(dop_hbm, dopx.at[pl.ds(3, planes)], own_sem.at[0]),
        pltpu.make_async_copy(scr_hbm, scrx.at[pl.ds(2, planes)], own_sem.at[1]),
        pltpu.make_async_copy(qw_hbm, qw_ref, own_sem.at[5]),
        pltpu.make_async_copy(slot_hbm, slot_ref, own_sem.at[6]),
        pltpu.make_async_copy(plane_hbm, plane_ref, own_sem.at[7]),
    ]
    for copy in own:
        copy.start()

    barrier = pltpu.get_barrier_semaphore()
    extra_up = jnp.logical_and(layer == n_layer - 1, energy < n_energy - 1)
    extra_down = jnp.logical_and(layer == 0, energy > 0)
    for k in range(1, nz):
        pl.semaphore_signal(barrier, inc=1, device_id=z_dev(lax.rem(z + k, nz)), device_id_type=MESH)
    for k in range(1, n_plane):
        pl.semaphore_signal(barrier, inc=1, device_id=plane_dev(lax.rem(here + k, n_plane)), device_id_type=MESH)

    @pl.when(extra_up)
    def _():
        pl.semaphore_signal(barrier, inc=1, device_id=slab_dev(slab + 1), device_id_type=MESH)

    @pl.when(extra_down)
    def _():
        pl.semaphore_signal(barrier, inc=1, device_id=slab_dev(slab - 1), device_id_type=MESH)

    t_load.wait()
    for q, value in enumerate((t_ref[...], t_ref[...].T)):
        t_both[q] = value
        t_b[q] = value.astype(BF16)

    rows = lax.broadcasted_iota(jnp.int32, (size, size), 0)
    cols = lax.broadcasted_iota(jnp.int32, (size, size), 1)

    def diagonal(mat):
        return jnp.sum(jnp.where(rows == cols, mat, 0.0), axis=0, keepdims=True)

    def propagator(q, i):
        d = inv[layer_at(q, i)]
        on = jnp.where(rows == cols, d, 0.0)
        down = jnp.sum(on, axis=1, keepdims=True)
        along = jnp.sum(on, axis=0, keepdims=True)
        off = [jnp.where(rows == cols, 0.0, d).astype(BF16)]
        p = down * t_both[q] + mm(off, [t_b[q]])
        pt = along * t_both[1 - q] + mm([t_b[1 - q]], off)
        return p, pt

    def pieces(p, pt):
        return parts_of(p, MOVE[0]), parts_of(pt, max(PULL[1], CARRY[1]))

    def begin(q):
        l = layer_at(q, 0)
        k = propagator(q, 0)[1]
        k_ref[q, l] = k
        return inv[l], k, pieces(*propagator(q, 1))

    def step(q, i, chain):
        s, k, (p, pt) = chain
        l = layer_at(q, i)
        y_mat = mm(parts_of(s, PULL[0]), pt[: PULL[1]])
        k = mm(parts_of(k, CARRY[0]), pt[: CARRY[1]])
        ahead = pieces(*propagator(q, i + 1)) if i + 1 < count else None
        moved = mm(p, parts_of(y_mat, MOVE[1]))
        k_ref[q, l] = k
        s = inv[l] + moved
        acc[pl.ds(l, 1), :] = acc[pl.ds(l, 1), :] + diagonal(moved)
        if i + 1 == count:
            s_ref[q] = s
        return s, k, ahead

    def halo_up():
        dev = slab_dev(slab + 1)
        return [
            pltpu.make_async_remote_copy(
                dop_hbm.at[pl.ds(planes - 3, 3)], dopx.at[pl.ds(0, 3)],
                halo_send.at[0], halo_recv.at[0], device_id=dev, device_id_type=MESH),
            pltpu.make_async_remote_copy(
                scr_hbm.at[pl.ds(planes - 2, 2)], scrx.at[pl.ds(0, 2)],
                halo_send.at[1], halo_recv.at[1], device_id=dev, device_id_type=MESH),
        ]

    def halo_down():
        dev = slab_dev(slab - 1)
        return [
            pltpu.make_async_remote_copy(
                dop_hbm.at[pl.ds(0, 3)], dopx.at[pl.ds(planes + 3, 3)],
                halo_send.at[2], halo_recv.at[2], device_id=dev, device_id_type=MESH),
            pltpu.make_async_remote_copy(
                scr_hbm.at[pl.ds(0, 2)], scrx.at[pl.ds(planes + 2, 2)],
                halo_send.at[3], halo_recv.at[3], device_id=dev, device_id_type=MESH),
        ]

    has_up = slab < n_slabs - 1
    has_down = slab > 0

    half = size // 2
    r_half = lax.broadcasted_iota(jnp.int32, (half, half), 0)
    c_half = lax.broadcasted_iota(jnp.int32, (half, half), 1)

    def pack(q, mat):
        one, two = mat[:half, :half], mat[half:, half:]
        wire_out[q, 0:half] = mat[:half, half:]
        wire_out[q, half:size] = jnp.where(r_half <= c_half, one, two)
        line = jnp.sum(jnp.where(r_half == c_half, two, 0.0), axis=0, keepdims=True)
        wire_out[q, size : size + 8] = jnp.broadcast_to(line, (8, half))

    def unpack(q):
        side, both = wire_in[q, 0:half], wire_in[q, half:size]
        over = both.T
        line = wire_in[q, size : size + 1]
        e_ref[q, 0:half, half:size] = side
        e_ref[q, half:size, 0:half] = side.T
        e_ref[q, 0:half, 0:half] = jnp.where(r_half <= c_half, both, over)
        two = jnp.where(r_half > c_half, both, over)
        e_ref[q, half:size, half:size] = jnp.where(r_half == c_half, line, two)

    def relay(q):
        dev = plane_dev(here + 1 - 2 * q)
        return pltpu.make_async_remote_copy(
            wire_out.at[q], wire_in.at[q], relay_send.at[q], relay_recv.at[q], device_id=dev, device_id_type=MESH
        )

    def row_of(q, eb, l):
        k_here = k_ref[q, l]
        g = mm(eb, parts_of(k_here, ENTER[1]))
        return k_here, g, jnp.sum(g * k_here, axis=0, keepdims=True)

    def add_row(l, row):
        acc[pl.ds(l, 1), :] = acc[pl.ds(l, 1), :] + row

    def pass_on(q):
        at_end = layer == (1 - q) * (n_layer - 1)
        l = layer_at(q, count - 1)
        k_last, g, row = row_of(q, parts_of(e_ref[q], ENTER[0]), l)

        @pl.when(jnp.logical_not(at_end))
        def _():
            pack(q, s_ref[q] + mm(parts_of(k_last.T, LEAVE[0]), parts_of(g, LEAVE[1])))
            relay(q).start()

        add_row(l, row)

    def rest(q):
        eb = parts_of(e_ref[q], ENTER[0])
        found = [row_of(q, eb, layer_at(q, i))[2] for i in range(count - 1)]
        for i, row in enumerate(found):
            add_row(layer_at(q, i), row)

    second = 1 - first
    for i in range(2):
        l = layer_at(first, i)
        pltpu.make_async_copy(inv_hbm.at[l], inv.at[l], inv_sem.at[l]).wait()
    chain = begin(first)
    for i in range(2, count):
        l = layer_at(first, i)
        pltpu.make_async_copy(inv_hbm.at[l], inv.at[l], inv_sem.at[l]).wait()
    for i in range(count):
        acc[i : i + 1, :] = diagonal(inv[i])
    outer = jnp.logical_or(*edges)
    inner_seg = jnp.logical_not(outer)

    def start_halos():
        @pl.when(has_up)
        def _():
            for copy in halo_up():
                copy.start()

        @pl.when(has_down)
        def _():
            for copy in halo_down():
                copy.start()

    for i in range(1, MEET):
        chain = step(first, i, chain)

    more = jnp.where(extra_up, 1, 0) + jnp.where(extra_down, 1, 0)
    pl.semaphore_wait(barrier, nz - 1 + n_plane - 1 + more)
    pl.when(outer)(start_halos)

    for i in range(MEET, count):
        chain = step(first, i, chain)
    for edge, copy in zip(edges, lead_loads):
        pl.when(edge)(copy.wait)

    @pl.when(outer)
    def _():
        pass_on(first)

    chain = begin(second)
    for i in range(1, 1 + EARLY):
        chain = step(second, i, chain)

    @pl.when(inner_seg)
    def _():
        relay(first).wait_recv()
        unpack(first)
        pass_on(first)

    for i in range(1 + EARLY, count):
        chain = step(second, i, chain)

    @pl.when(outer)
    def _():
        rest(first)

    relay(second).wait_recv()
    unpack(second)
    pass_on(second)

    @pl.when(inner_seg)
    def _():
        start_halos()
        rest(first)

    rest(second)

    for copy in own:
        copy.wait()
    slots = lax.broadcasted_iota(jnp.int32, qw_ref.shape, 1)
    weight = jnp.sum(jnp.where(slots == slot_ref[...], qw_ref[...], 0.0), axis=1, keepdims=True)
    part[...] = weight * acc[...]

    along_z = (nz, z, z_dev)
    in_plane = (n_plane, here, plane_dev)

    def copies(group, src, buf, send, recv, arriving):
        number, me, device = group
        for k in range(1, number):
            other = lax.rem(me + k, number)
            slot = other if arriving else me
            yield pltpu.make_async_remote_copy(
                src, buf.at[slot], send.at[other], recv.at[slot], device_id=device(other), device_id_type=MESH
            )

    def exchange(group, src, buf, send, recv):
        for copy in copies(group, src, buf, send, recv, False):
            copy.start()
        buf[group[1]] = src[...]
        for copy in copies(group, src, buf, send, recv, True):
            copy.wait_recv()

    def total_of(buf, slots):
        total = None
        for k in slots:
            total = buf[k] if total is None else total + buf[k]
        return total

    exchange(along_z, part, zbuf, zs, zr)
    psrc[...] = total_of(zbuf, range(nz))
    exchange(in_plane, psrc, pbuf, ps, pr)
    gathered = [total_of(pbuf, range(lay, n_plane, n_layer)) for lay in range(n_layer)]
    dens = jnp.concatenate(gathered, axis=0)
    mine = gathered[0]
    for lay in range(1, n_layer):
        mine = jnp.where(layer == lay, gathered[lay], mine)
    dens_out[...] = mine

    @pl.when(has_down)
    def _():
        for copy in halo_up():
            copy.wait_recv()

    @pl.when(has_up)
    def _():
        for copy in halo_down():
            copy.wait_recv()

    @pl.when(jnp.logical_not(has_down))
    def _():
        dopx[0:3] = jnp.zeros((3, *dopx.shape[1:]), F32)
        scrx[0:2] = jnp.zeros((2, *scrx.shape[1:]), F32)

    @pl.when(jnp.logical_not(has_up))
    def _():
        dopx[planes + 3 : planes + 6] = jnp.zeros((3, *dopx.shape[1:]), F32)
        scrx[planes + 2 : planes + 4] = jnp.zeros((2, *scrx.shape[1:]), F32)

    low = slab * planes - 3
    n_near = planes + 6
    near = 16
    ids = low + lax.broadcasted_iota(jnp.int32, (near, plane_ref.shape[1]), 0)
    onehot = jnp.where(plane_ref[...] == ids, 1.0, 0.0)
    pc = jnp.dot(onehot, dens, precision=HI, preferred_element_type=F32)
    n_side = dop_hbm.shape[2]
    cell = n_side // ORB
    spread_m = lax.broadcasted_iota(jnp.int32, (size, n_side), 0)
    spread_z = lax.broadcasted_iota(jnp.int32, (size, n_side), 1)
    spread = jnp.where(lax.rem(spread_m, ORB) == lax.div(spread_z, cell), 1.0, 0.0)
    row_j = lax.broadcasted_iota(jnp.int32, (ORB, size), 0)
    row_m = lax.broadcasted_iota(jnp.int32, (ORB, size), 1)
    own_row = row_j == lax.div(row_m, ORB)
    tall = jnp.concatenate([jnp.where(own_row, pc[q : q + 1, :], 0.0) for q in range(n_near)], axis=0)
    wide = jnp.dot(tall, spread, precision=HI, preferred_element_type=F32)
    n_y = dop_hbm.shape[1]
    for q in range(n_near):
        for j in range(ORB):
            row = wide[q * ORB + j : q * ORB + j + 1, :]
            where = pl.ds(j * (n_y // ORB), n_y // ORB)
            dopx[q, where, :] = row - dopx[q, where, :]

    at_y = lax.broadcasted_iota(jnp.int32, (n_y, n_side), 0)
    at_z = lax.broadcasted_iota(jnp.int32, (n_y, n_side), 1)

    def applied(src, dst, trim):
        n_dst = n_near - 2 * trim
        for q in range(n_dst):
            mid = src[q + 1]
            beside = src[q] + src[q + 2]
            beside = beside + jnp.where(at_y == 0, 0.0, pltpu.roll(mid, 1, 0))
            beside = beside + jnp.where(at_y == n_y - 1, 0.0, pltpu.roll(mid, n_y - 1, 0))
            beside = beside + jnp.where(at_z == 0, 0.0, pltpu.roll(mid, 1, 1))
            beside = beside + jnp.where(at_z == n_side - 1, 0.0, pltpu.roll(mid, n_side - 1, 1))
            value = (scrx[q + trim - 1] + (6.0 - SHIFT)) * mid - beside
            if q < 3 - trim:
                value = jnp.where(has_down, value, 0.0)
            if q >= 3 - trim + planes:
                value = jnp.where(has_up, value, 0.0)
            dst[q] = value

    applied(dopx, u1, 1)
    applied(u1, u2, 2)
    applied(u2, u3, 3)

    def inner(a, a0, b, b0):
        total = None
        for q in range(planes):
            term = a[a0 + q] * b[b0 + q]
            total = term if total is None else total + term
        return jnp.sum(jnp.sum(total, axis=0, keepdims=True), axis=1, keepdims=True)

    sums = [
        inner(dopx, 3, dopx, 3), inner(dopx, 3, u1, 2), inner(u1, 2, u1, 2),
        inner(u1, 2, u2, 1), inner(u2, 1, u2, 1), inner(u2, 1, u3, 0),
    ]
    lane = lax.broadcasted_iota(jnp.int32, (1, 128), 1)
    row = jnp.zeros((1, 128), F32)
    for k, value in enumerate(sums):
        row = jnp.where(lane == k, value, row)
    mom[...] = row
    exchange(along_z, mom, zmom, mzs, mzr)
    msrc[...] = total_of(zmom, range(nz))
    exchange(in_plane, msrc, pmom, mps, mpr)
    total = total_of(pmom, range(n_plane))
    moment = [total[:, k : k + 1] for k in range(6)]

    def product(a, b):
        value = None
        for i, p in enumerate(a):
            for j, q in enumerate(b):
                term = p * q * moment[i + j]
                value = term if value is None else value + term
        return value

    def times_a(a):
        shifted = [None, *a]
        kept = [SHIFT * v for v in a] + [None]
        return [w if v is None else v if w is None else v + w for v, w in zip(shifted, kept)]

    def plus(a, factor, b):
        longest = max(len(a), len(b))
        result = []
        for i in range(longest):
            if i >= len(b):
                result.append(a[i])
            elif i >= len(a):
                result.append(factor * b[i])
            else:
                result.append(a[i] + factor * b[i])
        return result

    one = jnp.ones((1, 1), F32)
    residual, direction, potential = [one], [one], []
    norm = moment[0]
    for iteration in range(CG_ITERS):
        a_dir = times_a(direction)
        step_size = norm / product(direction, a_dir)
        potential = plus(potential, step_size, direction)
        residual = plus(residual, -step_size, a_dir)
        if iteration + 1 < CG_ITERS:
            new = product(residual, residual)
            direction = plus(residual, new / norm, direction)
            norm = new

    for q in range(planes):
        v = [dopx[3 + q], u1[2 + q], u2[1 + q], u3[q]]
        x = potential[0] * v[0]
        for k in range(1, CG_ITERS):
            x = x + potential[k] * v[k]
        pot_out[q] = x
        r = residual[0] * v[0]
        for k in range(1, CG_ITERS + 1):
            r = r + residual[k] * v[k]
        res_out[q] = r

    for sent in (
        (along_z, part, zbuf, zs, zr), (in_plane, psrc, pbuf, ps, pr),
        (along_z, mom, zmom, mzs, mzr), (in_plane, msrc, pmom, mps, mpr),
    ):
        for copy in copies(*sent, False):
            copy.wait_send()

    relay(first).wait_send()

    @pl.when(inner_seg)
    def _():
        relay(second).wait_send()

    @pl.when(has_up)
    def _():
        for copy in halo_up():
            copy.wait_send()

    @pl.when(has_down)
    def _():
        for copy in halo_down():
            copy.wait_send()


def body(
    sizes,
    layer_inverse,
    coupling,
    lead_left,
    lead_right,
    quad_weight,
    energy_slot,
    plane_of,
    doping,
    screening,
):
    ny, nxl, nz, nxh, nc = sizes
    _, count, size, _ = layer_inverse.shape
    planes, n_y, n_z = doping.shape
    n_plane = ny * nxl * nxh * nc
    vmem = pl.BlockSpec(memory_space=pltpu.VMEM)
    hbm = pl.BlockSpec(memory_space=pltpu.HBM)
    square = pltpu.VMEM((size, size), F32)
    squares = pltpu.VMEM((count, size, size), F32)
    dma = pltpu.SemaphoreType.DMA
    rows = pltpu.VMEM((count, size), F32)
    operands = (
        layer_inverse[0], coupling, lead_left[0], lead_right[0], quad_weight[None], energy_slot[None], plane_of[None],
        doping, screening,
    )
    return pl.pallas_call(
        functools.partial(kernel, sizes),
        out_shape=(
            jax.ShapeDtypeStruct((count, size), F32),
            jax.ShapeDtypeStruct(doping.shape, F32),
            jax.ShapeDtypeStruct(doping.shape, F32),
        ),
        in_specs=[hbm] * 9,
        out_specs=(vmem, vmem, vmem),
        scratch_shapes=[
            squares,
            square,
            pltpu.VMEM((2, size, size), F32),
            pltpu.VMEM((2, size, size), BF16),
            pltpu.VMEM((2, size, size), F32),
            pltpu.VMEM((2, count, size, size), F32),
            rows,
            pltpu.VMEM((2, size, size), F32),
            pltpu.VMEM((2, size + 8, size // 2), F32),
            pltpu.VMEM((2, size + 8, size // 2), F32),
            pltpu.VMEM((1, quad_weight.shape[0]), F32),
            pltpu.VMEM((1, 1), jnp.int32),
            pltpu.VMEM((1, plane_of.shape[0]), jnp.int32),
            pltpu.VMEM((planes + 6, n_y, n_z), F32),
            pltpu.VMEM((planes + 4, n_y, n_z), F32),
            pltpu.VMEM((planes + 4, n_y, n_z), F32),
            pltpu.VMEM((planes + 2, n_y, n_z), F32),
            pltpu.VMEM((planes, n_y, n_z), F32),
            rows,
            pltpu.VMEM((nz, count, size), F32),
            rows,
            pltpu.VMEM((n_plane, count, size), F32),
            pltpu.VMEM((1, 128), F32),
            pltpu.VMEM((nz, 1, 128), F32),
            pltpu.VMEM((n_plane, 1, 128), F32),
            pltpu.VMEM((1, 128), F32),
            dma((count,)), dma((8,)), dma((4,)), dma((4,)), dma((2,)), dma((2,)),
            dma((nz,)), dma((nz,)), dma((n_plane,)), dma((n_plane,)),
            dma((nz,)), dma((nz,)), dma((n_plane,)), dma((n_plane,)),
        ],
        compiler_params=pltpu.CompilerParams(
            collective_id=0, has_side_effects=True, vmem_limit_bytes=VMEM
        ),
    )(*[v if v.size == 1 else pltpu.with_memory_space_constraint(v, pltpu.HBM) for v in operands])


def sharded(split):
    energy_layer = (*ENERGY, *LAYER)
    in_specs = (
        P(ENERGY, LAYER, None, None),
        P(),
        P(ENERGY, None, None),
        P(ENERGY, None, None),
        P(),
        P(ENERGY),
        P(),
        P(energy_layer, None, None),
        P(energy_layer, None, None),
    )
    out_specs = (P(LAYER, None), P(energy_layer, None, None), P(energy_layer, None, None))
    sizes = tuple(split.shape[a] for a in AXES)
    return jax.shard_map(
        functools.partial(body, sizes), mesh=split, in_specs=in_specs, out_specs=out_specs, check_vma=False
    )


def solution(mesh):
    return sharded(Mesh(mesh.devices.reshape(4, 2, 8, 2, 2), AXES))
```

```python
import functools
import itertools

import jax
import jax.numpy as jnp
from jax import lax
from jax.experimental import pallas as pl
from jax.experimental.pallas import tpu as pltpu
from jax.sharding import Mesh
from jax.sharding import PartitionSpec as P

AXES = ("energy_0", "energy_1", "energy_2", "layer_0", "layer_1")
LAYER = ("layer_0", "layer_1")
ENERGY = ("energy_0", "energy_1", "energy_2")
ORB = 16
CG_ITERS = 3
SHIFT = 7.0
VMEM = 48 * 1024 * 1024
PULL = (1, 2)
CARRY = (1, 2)
MOVE = (2, 1)
ENTER = (1, 1)
LEAVE = (1, 1)
EARLY = 1
MEET = 6
MESH = pl.DeviceIdType.MESH
HI = lax.Precision.HIGHEST
F32 = jnp.float32
BF16 = jnp.bfloat16


def parts_of(x, count):
    parts = []
    for _ in range(count):
        part = x.astype(BF16)
        parts.append(part)
        x = x - part.astype(F32)
    return parts


def mm(left, right):
    total = None
    most = max(len(left), len(right))
    for i, a in enumerate(left):
        for j, b in enumerate(right):
            if i + j < most:
                term = jnp.dot(a, b, preferred_element_type=F32)
                total = term if total is None else total + term
    return total


def kernel(
    sizes,
    inv_hbm, t_hbm, lead_l, lead_r, qw_hbm, slot_hbm, plane_hbm, dop_hbm, scr_hbm,
    dens_out, both_out,
    inv, t_ref, t_both, t_b, s_ref, k_ref, acc, e_ref, wire_in, wire_out, qw_ref, slot_ref, plane_ref,
    dopx, scrx, u1, u2, u3, part, zbuf, psrc, pbuf, mom, zmom, pmom, msrc,
    inv_sem, own_sem, halo_send, halo_recv, relay_send, relay_recv,
    zs, zr, ps, pr, mzs, mzr, mps, mpr,
):
    ny, nxl, nz, nxh, nc = sizes
    y, xl, z, xh, c = [lax.axis_index(a) for a in AXES]
    n_layer = nxh * nc
    n_plane = ny * nxl * n_layer
    n_energy = ny * nxl * nz
    layer = xh * nc + c
    energy = (y * nxl + xl) * nz + z
    slab = energy * n_layer + layer
    n_slabs = n_energy * n_layer
    here = (y * nxl + xl) * n_layer + layer
    count, size, _ = inv_hbm.shape
    planes = dop_hbm.shape[0]

    on_y, on_xl, on_z, on_xh, on_c = [
        [lax.rem(at + k, length) for k in range(length)] for at, length in zip((y, xl, z, xh, c), sizes)
    ]

    def around(k, length):
        return min(k, length - k)

    steps = sorted(
        itertools.product(range(ny), range(nxl), range(nxh), range(nc)),
        key=lambda k: -(around(k[0], ny) + k[1] + 2 * k[2]),
    )
    plane_peers = [
        (on_y[k[0]], on_xl[k[1]], z, on_xh[k[2]], on_c[k[3]]) for k in steps if any(k)
    ]
    line_peers = [(y, xl, on_z[k], xh, c) for k in sorted(range(1, nz), key=lambda k: -around(k, nz))]

    first = jnp.where(layer >= n_layer // 2, 1, 0)

    def layer_at(q, i):
        return q * (count - 1) + (1 - 2 * q) * i

    t_load = pltpu.make_async_copy(t_hbm, t_ref, own_sem.at[2])
    t_load.start()
    for i in range(count):
        l = layer_at(first, i)
        pltpu.make_async_copy(inv_hbm.at[l], inv.at[l], inv_sem.at[l]).start()
    lead_loads = [
        pltpu.make_async_copy(lead_l, e_ref.at[0], own_sem.at[3]),
        pltpu.make_async_copy(lead_r, e_ref.at[1], own_sem.at[4]),
    ]
    edges = [layer == 0, layer == n_layer - 1]
    for edge, copy in zip(edges, lead_loads):
        pl.when(edge)(copy.start)
    own = [
        pltpu.make_async_copy(dop_hbm, dopx.at[pl.ds(3, planes)], own_sem.at[0]),
        pltpu.make_async_copy(scr_hbm, scrx.at[pl.ds(2, planes)], own_sem.at[1]),
        pltpu.make_async_copy(qw_hbm, qw_ref, own_sem.at[5]),
        pltpu.make_async_copy(slot_hbm, slot_ref, own_sem.at[6]),
        pltpu.make_async_copy(plane_hbm, plane_ref, own_sem.at[7]),
    ]
    for copy in own:
        copy.start()

    def slab_dev(index):
        en, lay = lax.div(index, n_layer), lax.rem(index, n_layer)
        group, zz = lax.div(en, nz), lax.rem(en, nz)
        return (lax.div(group, nxl), lax.rem(group, nxl), zz, lax.div(lay, nc), lax.rem(lay, nc))

    slab_up = slab_dev(jnp.minimum(slab + 1, n_slabs - 1))
    slab_down = slab_dev(jnp.maximum(slab - 1, 0))

    barrier = pltpu.get_barrier_semaphore()
    extra_up = jnp.logical_and(layer == n_layer - 1, energy < n_energy - 1)
    extra_down = jnp.logical_and(layer == 0, energy > 0)
    for peer in line_peers + plane_peers:
        pl.semaphore_signal(barrier, inc=1, device_id=peer, device_id_type=MESH)

    @pl.when(extra_up)
    def _():
        pl.semaphore_signal(barrier, inc=1, device_id=slab_up, device_id_type=MESH)

    @pl.when(extra_down)
    def _():
        pl.semaphore_signal(barrier, inc=1, device_id=slab_down, device_id_type=MESH)

    t_load.wait()
    for q, value in enumerate((t_ref[...], t_ref[...].T)):
        t_both[q] = value
        t_b[q] = value.astype(BF16)

    rows = lax.broadcasted_iota(jnp.int32, (size, size), 0)
    cols = lax.broadcasted_iota(jnp.int32, (size, size), 1)

    def diagonal(mat):
        return jnp.sum(jnp.where(rows == cols, mat, 0.0), axis=0, keepdims=True)

    def propagator(q, i):
        d = inv[layer_at(q, i)]
        on = jnp.where(rows == cols, d, 0.0)
        down = jnp.sum(on, axis=1, keepdims=True)
        along = jnp.sum(on, axis=0, keepdims=True)
        off = [jnp.where(rows == cols, 0.0, d).astype(BF16)]
        p = down * t_both[q] + mm(off, [t_b[q]])
        pt = along * t_both[1 - q] + mm([t_b[1 - q]], off)
        return p, pt

    def pieces(p, pt):
        return parts_of(p, MOVE[0]), parts_of(pt, max(PULL[1], CARRY[1]))

    def begin(q):
        l = layer_at(q, 0)
        k = propagator(q, 0)[1]
        k_ref[q, l] = k
        return inv[l], k, pieces(*propagator(q, 1))

    def step(q, i, chain):
        s, k, (p, pt) = chain
        l = layer_at(q, i)
        y_mat = mm(parts_of(s, PULL[0]), pt[: PULL[1]])
        k = mm(parts_of(k, CARRY[0]), pt[: CARRY[1]])
        ahead = pieces(*propagator(q, i + 1)) if i + 1 < count else None
        moved = mm(p, parts_of(y_mat, MOVE[1]))
        k_ref[q, l] = k
        s = inv[l] + moved
        acc[pl.ds(l, 1), :] = acc[pl.ds(l, 1), :] + diagonal(moved)
        if i + 1 == count:
            s_ref[q] = s
        return s, k, ahead

    def halo_up():
        dev = slab_up
        return [
            pltpu.make_async_remote_copy(
                dop_hbm.at[pl.ds(planes - 3, 3)], dopx.at[pl.ds(0, 3)],
                halo_send.at[0], halo_recv.at[0], device_id=dev, device_id_type=MESH),
            pltpu.make_async_remote_copy(
                scr_hbm.at[pl.ds(planes - 2, 2)], scrx.at[pl.ds(0, 2)],
                halo_send.at[1], halo_recv.at[1], device_id=dev, device_id_type=MESH),
        ]

    def halo_down():
        dev = slab_down
        return [
            pltpu.make_async_remote_copy(
                dop_hbm.at[pl.ds(0, 3)], dopx.at[pl.ds(planes + 3, 3)],
                halo_send.at[2], halo_recv.at[2], device_id=dev, device_id_type=MESH),
            pltpu.make_async_remote_copy(
                scr_hbm.at[pl.ds(0, 2)], scrx.at[pl.ds(planes + 2, 2)],
                halo_send.at[3], halo_recv.at[3], device_id=dev, device_id_type=MESH),
        ]

    has_up = slab < n_slabs - 1
    has_down = slab > 0

    half = size // 2
    r_half = lax.broadcasted_iota(jnp.int32, (half, half), 0)
    c_half = lax.broadcasted_iota(jnp.int32, (half, half), 1)

    def pack(q, mat):
        one, two = mat[:half, :half], mat[half:, half:]
        wire_out[q, 0:half] = mat[:half, half:]
        wire_out[q, half:size] = jnp.where(r_half <= c_half, one, two)
        line = jnp.sum(jnp.where(r_half == c_half, two, 0.0), axis=0, keepdims=True)
        wire_out[q, size : size + 8] = jnp.broadcast_to(line, (8, half))

    def unpack(q):
        side, both = wire_in[q, 0:half], wire_in[q, half:size]
        over = both.T
        line = wire_in[q, size : size + 1]
        e_ref[q, 0:half, half:size] = side
        e_ref[q, half:size, 0:half] = side.T
        e_ref[q, 0:half, 0:half] = jnp.where(r_half <= c_half, both, over)
        two = jnp.where(r_half > c_half, both, over)
        e_ref[q, half:size, half:size] = jnp.where(r_half == c_half, line, two)

    def relay(q):
        to = jnp.clip(layer + 1 - 2 * q, 0, n_layer - 1)
        dev = (y, xl, z, lax.div(to, nc), lax.rem(to, nc))
        return pltpu.make_async_remote_copy(
            wire_out.at[q], wire_in.at[q], relay_send.at[q], relay_recv.at[q], device_id=dev, device_id_type=MESH
        )

    def row_of(q, eb, l):
        k_here = k_ref[q, l]
        g = mm(eb, parts_of(k_here, ENTER[1]))
        return k_here, g, jnp.sum(g * k_here, axis=0, keepdims=True)

    def add_row(l, row):
        acc[pl.ds(l, 1), :] = acc[pl.ds(l, 1), :] + row

    def pass_on(q):
        at_end = layer == (1 - q) * (n_layer - 1)
        l = layer_at(q, count - 1)
        k_last, g, row = row_of(q, parts_of(e_ref[q], ENTER[0]), l)

        @pl.when(jnp.logical_not(at_end))
        def _():
            pack(q, s_ref[q] + mm(parts_of(k_last.T, LEAVE[0]), parts_of(g, LEAVE[1])))
            relay(q).start()

        add_row(l, row)

    def rest(q):
        eb = parts_of(e_ref[q], ENTER[0])
        found = [row_of(q, eb, layer_at(q, i))[2] for i in range(count - 1)]
        for i, row in enumerate(found):
            add_row(layer_at(q, i), row)

    second = 1 - first
    for i in range(2):
        l = layer_at(first, i)
        pltpu.make_async_copy(inv_hbm.at[l], inv.at[l], inv_sem.at[l]).wait()
    chain = begin(first)
    for i in range(2, count):
        l = layer_at(first, i)
        pltpu.make_async_copy(inv_hbm.at[l], inv.at[l], inv_sem.at[l]).wait()
    for i in range(count):
        acc[i : i + 1, :] = diagonal(inv[i])
    outer = jnp.logical_or(*edges)
    inner_seg = jnp.logical_not(outer)

    def start_halos():
        @pl.when(has_up)
        def _():
            for copy in halo_up():
                copy.start()

        @pl.when(has_down)
        def _():
            for copy in halo_down():
                copy.start()

    for i in range(1, MEET):
        chain = step(first, i, chain)

    more = jnp.where(extra_up, 1, 0) + jnp.where(extra_down, 1, 0)
    pl.semaphore_wait(barrier, nz - 1 + n_plane - 1 + more)

    for i in range(MEET, count):
        chain = step(first, i, chain)
    for edge, copy in zip(edges, lead_loads):
        pl.when(edge)(copy.wait)

    @pl.when(outer)
    def _():
        pass_on(first)

    chain = begin(second)
    for i in range(1, 1 + EARLY):
        chain = step(second, i, chain)

    @pl.when(inner_seg)
    def _():
        relay(first).wait_recv()
        unpack(first)
        pass_on(first)

    for i in range(1 + EARLY, count):
        chain = step(second, i, chain)

    @pl.when(outer)
    def _():
        start_halos()
        rest(first)

    relay(second).wait_recv()
    unpack(second)
    pass_on(second)

    @pl.when(inner_seg)
    def _():
        start_halos()
        rest(first)

    rest(second)

    for copy in own:
        copy.wait()
    slots = lax.broadcasted_iota(jnp.int32, qw_ref.shape, 1)
    weight = jnp.sum(jnp.where(slots == slot_ref[...], qw_ref[...], 0.0), axis=1, keepdims=True)
    part[...] = weight * acc[...]

    along_z = (z, line_peers)
    in_plane = (here, plane_peers)

    def exchange(group, src, buf, send, recv):
        me, peers = group
        for peer in peers:
            pltpu.make_async_remote_copy(
                src, buf.at[me], send, recv, device_id=peer, device_id_type=MESH
            ).start()
        buf[me] = src[...]
        all_of(group, src, buf, send, recv).wait_recv()

    def all_of(group, src, buf, send, recv):
        most = pl.ds(0, len(group[1]))
        return pltpu.make_async_remote_copy(
            buf.at[most], buf.at[most], send, recv, device_id=group[1][0], device_id_type=MESH
        )

    def total_of(buf, slots):
        total = None
        for k in slots:
            total = buf[k] if total is None else total + buf[k]
        return total

    exchange(along_z, part, zbuf, zs, zr)
    psrc[...] = total_of(zbuf, range(nz))
    exchange(in_plane, psrc, pbuf, ps, pr)
    gathered = [total_of(pbuf, range(lay, n_plane, n_layer)) for lay in range(n_layer)]
    dens = jnp.concatenate(gathered, axis=0)
    mine = gathered[0]
    for lay in range(1, n_layer):
        mine = jnp.where(layer == lay, gathered[lay], mine)
    dens_out[...] = mine

    @pl.when(has_down)
    def _():
        for copy in halo_up():
            copy.wait_recv()

    @pl.when(has_up)
    def _():
        for copy in halo_down():
            copy.wait_recv()

    @pl.when(jnp.logical_not(has_down))
    def _():
        dopx[0:3] = jnp.zeros((3, *dopx.shape[1:]), F32)
        scrx[0:2] = jnp.zeros((2, *scrx.shape[1:]), F32)

    @pl.when(jnp.logical_not(has_up))
    def _():
        dopx[planes + 3 : planes + 6] = jnp.zeros((3, *dopx.shape[1:]), F32)
        scrx[planes + 2 : planes + 4] = jnp.zeros((2, *scrx.shape[1:]), F32)

    low = slab * planes - 3
    n_near = planes + 6
    near = 16
    ids = low + lax.broadcasted_iota(jnp.int32, (near, plane_ref.shape[1]), 0)
    onehot = jnp.where(plane_ref[...] == ids, 1.0, 0.0)
    pc = jnp.dot(onehot, dens, precision=HI, preferred_element_type=F32)
    n_side = dop_hbm.shape[2]
    cell = n_side // ORB
    spread_m = lax.broadcasted_iota(jnp.int32, (size, n_side), 0)
    spread_z = lax.broadcasted_iota(jnp.int32, (size, n_side), 1)
    spread = jnp.where(lax.rem(spread_m, ORB) == lax.div(spread_z, cell), 1.0, 0.0)
    row_j = lax.broadcasted_iota(jnp.int32, (ORB, size), 0)
    row_m = lax.broadcasted_iota(jnp.int32, (ORB, size), 1)
    own_row = row_j == lax.div(row_m, ORB)
    tall = jnp.concatenate([jnp.where(own_row, pc[q : q + 1, :], 0.0) for q in range(n_near)], axis=0)
    wide = jnp.dot(tall, spread, precision=HI, preferred_element_type=F32)
    n_y = dop_hbm.shape[1]
    for q in range(n_near):
        for j in range(ORB):
            row = wide[q * ORB + j : q * ORB + j + 1, :]
            where = pl.ds(j * (n_y // ORB), n_y // ORB)
            dopx[q, where, :] = row - dopx[q, where, :]

    at_y = lax.broadcasted_iota(jnp.int32, (n_y, n_side), 0)
    at_z = lax.broadcasted_iota(jnp.int32, (n_y, n_side), 1)

    def applied(src, dst, trim):
        n_dst = n_near - 2 * trim
        for q in range(n_dst):
            mid = src[q + 1]
            beside = src[q] + src[q + 2]
            beside = beside + jnp.where(at_y == 0, 0.0, pltpu.roll(mid, 1, 0))
            beside = beside + jnp.where(at_y == n_y - 1, 0.0, pltpu.roll(mid, n_y - 1, 0))
            beside = beside + jnp.where(at_z == 0, 0.0, pltpu.roll(mid, 1, 1))
            beside = beside + jnp.where(at_z == n_side - 1, 0.0, pltpu.roll(mid, n_side - 1, 1))
            value = (scrx[q + trim - 1] + (6.0 - SHIFT)) * mid - beside
            if q < 3 - trim:
                value = jnp.where(has_down, value, 0.0)
            if q >= 3 - trim + planes:
                value = jnp.where(has_up, value, 0.0)
            dst[q] = value

    applied(dopx, u1, 1)
    applied(u1, u2, 2)
    applied(u2, u3, 3)

    def inner(a, a0, b, b0):
        total = None
        for q in range(planes):
            term = a[a0 + q] * b[b0 + q]
            total = term if total is None else total + term
        return jnp.sum(jnp.sum(total, axis=0, keepdims=True), axis=1, keepdims=True)

    sums = [
        inner(dopx, 3, dopx, 3), inner(dopx, 3, u1, 2), inner(u1, 2, u1, 2),
        inner(u1, 2, u2, 1), inner(u2, 1, u2, 1), inner(u2, 1, u3, 0),
    ]
    lane = lax.broadcasted_iota(jnp.int32, (1, 128), 1)
    row = jnp.zeros((1, 128), F32)
    for k, value in enumerate(sums):
        row = jnp.where(lane == k, value, row)
    mom[...] = row
    exchange(along_z, mom, zmom, mzs, mzr)
    msrc[...] = total_of(zmom, range(nz))
    exchange(in_plane, msrc, pmom, mps, mpr)
    total = total_of(pmom, range(n_plane))
    moment = [total[:, k : k + 1] for k in range(6)]

    def product(a, b):
        value = None
        for i, p in enumerate(a):
            for j, q in enumerate(b):
                term = p * q * moment[i + j]
                value = term if value is None else value + term
        return value

    def times_a(a):
        shifted = [None, *a]
        kept = [SHIFT * v for v in a] + [None]
        return [w if v is None else v if w is None else v + w for v, w in zip(shifted, kept)]

    def plus(a, factor, b):
        longest = max(len(a), len(b))
        result = []
        for i in range(longest):
            if i >= len(b):
                result.append(a[i])
            elif i >= len(a):
                result.append(factor * b[i])
            else:
                result.append(a[i] + factor * b[i])
        return result

    one = jnp.ones((1, 1), F32)
    residual, direction, potential = [one], [one], []
    norm = moment[0]
    for iteration in range(CG_ITERS):
        a_dir = times_a(direction)
        step_size = norm / product(direction, a_dir)
        potential = plus(potential, step_size, direction)
        residual = plus(residual, -step_size, a_dir)
        if iteration + 1 < CG_ITERS:
            new = product(residual, residual)
            direction = plus(residual, new / norm, direction)
            norm = new

    for q in range(planes):
        v = [dopx[3 + q], u1[2 + q], u2[1 + q], u3[q]]
        x = potential[0] * v[0]
        for k in range(1, CG_ITERS):
            x = x + potential[k] * v[k]
        both_out[0, q] = x
        r = residual[0] * v[0]
        for k in range(1, CG_ITERS + 1):
            r = r + residual[k] * v[k]
        both_out[1, q] = r

    for sent in (
        (along_z, part, zbuf, zs, zr), (in_plane, psrc, pbuf, ps, pr),
        (along_z, mom, zmom, mzs, mzr), (in_plane, msrc, pmom, mps, mpr),
    ):
        all_of(*sent).wait_send()

    relay(first).wait_send()

    @pl.when(inner_seg)
    def _():
        relay(second).wait_send()

    @pl.when(has_up)
    def _():
        for copy in halo_up():
            copy.wait_send()

    @pl.when(has_down)
    def _():
        for copy in halo_down():
            copy.wait_send()


def body(
    sizes,
    layer_inverse,
    coupling,
    lead_left,
    lead_right,
    quad_weight,
    energy_slot,
    plane_of,
    doping,
    screening,
):
    ny, nxl, nz, nxh, nc = sizes
    _, count, size, _ = layer_inverse.shape
    planes, n_y, n_z = doping.shape
    n_plane = ny * nxl * nxh * nc
    vmem = pl.BlockSpec(memory_space=pltpu.VMEM)
    hbm = pl.BlockSpec(memory_space=pltpu.HBM)
    square = pltpu.VMEM((size, size), F32)
    squares = pltpu.VMEM((count, size, size), F32)
    dma = pltpu.SemaphoreType.DMA
    rows = pltpu.VMEM((count, size), F32)
    operands = (
        layer_inverse[0], coupling, lead_left[0], lead_right[0], quad_weight[None], energy_slot[None], plane_of[None],
        doping, screening,
    )
    dens, both = pl.pallas_call(
        functools.partial(kernel, sizes),
        out_shape=(
            jax.ShapeDtypeStruct((count, size), F32),
            jax.ShapeDtypeStruct((2, *doping.shape), F32),
        ),
        in_specs=[hbm] * 9,
        out_specs=(vmem, vmem),
        scratch_shapes=[
            squares,
            square,
            pltpu.VMEM((2, size, size), F32),
            pltpu.VMEM((2, size, size), BF16),
            pltpu.VMEM((2, size, size), F32),
            pltpu.VMEM((2, count, size, size), F32),
            rows,
            pltpu.VMEM((2, size, size), F32),
            pltpu.VMEM((2, size + 8, size // 2), F32),
            pltpu.VMEM((2, size + 8, size // 2), F32),
            pltpu.VMEM((1, quad_weight.shape[0]), F32),
            pltpu.VMEM((1, 1), jnp.int32),
            pltpu.VMEM((1, plane_of.shape[0]), jnp.int32),
            pltpu.VMEM((planes + 6, n_y, n_z), F32),
            pltpu.VMEM((planes + 4, n_y, n_z), F32),
            pltpu.VMEM((planes + 4, n_y, n_z), F32),
            pltpu.VMEM((planes + 2, n_y, n_z), F32),
            pltpu.VMEM((planes, n_y, n_z), F32),
            rows,
            pltpu.VMEM((nz, count, size), F32),
            rows,
            pltpu.VMEM((n_plane, count, size), F32),
            pltpu.VMEM((1, 128), F32),
            pltpu.VMEM((nz, 1, 128), F32),
            pltpu.VMEM((n_plane, 1, 128), F32),
            pltpu.VMEM((1, 128), F32),
            dma((count,)), dma((8,)), dma((4,)), dma((4,)), dma((2,)), dma((2,)),
            *[dma] * 8,
        ],
        compiler_params=pltpu.CompilerParams(
            collective_id=0, has_side_effects=True, vmem_limit_bytes=VMEM
        ),
    )(*[v if v.size == 1 else pltpu.with_memory_space_constraint(v, pltpu.HBM) for v in operands])
    return dens, both[0], both[1]


def sharded(split):
    energy_layer = (*ENERGY, *LAYER)
    in_specs = (
        P(ENERGY, LAYER, None, None),
        P(),
        P(ENERGY, None, None),
        P(ENERGY, None, None),
        P(),
        P(ENERGY),
        P(),
        P(energy_layer, None, None),
        P(energy_layer, None, None),
    )
    out_specs = (P(LAYER, None), P(energy_layer, None, None), P(energy_layer, None, None))
    sizes = tuple(split.shape[a] for a in AXES)
    return jax.shard_map(
        functools.partial(body, sizes), mesh=split, in_specs=in_specs, out_specs=out_specs, check_vma=False
    )


def solution(mesh):
    return sharded(Mesh(mesh.devices.reshape(4, 2, 8, 2, 2), AXES))
```

```python
import functools
import itertools

import jax
import jax.numpy as jnp
from jax import lax
from jax.experimental import pallas as pl
from jax.experimental.pallas import tpu as pltpu
from jax.sharding import Mesh
from jax.sharding import PartitionSpec as P

AXES = ("energy_0", "energy_1", "energy_2", "layer_0", "layer_1")
LAYER = ("layer_0", "layer_1")
ENERGY = ("energy_0", "energy_1", "energy_2")
ORB = 16
CG_ITERS = 3
SHIFT = 7.0
VMEM = 48 * 1024 * 1024
PULL = (1, 2)
CARRY = (1, 2)
MOVE = (2, 1)
ENTER = (1, 1)
LEAVE = (1, 1)
EARLY = 1
MESH = pl.DeviceIdType.MESH
HI = lax.Precision.HIGHEST
F32 = jnp.float32
BF16 = jnp.bfloat16


def parts_of(x, count):
    parts = []
    for _ in range(count):
        part = x.astype(BF16)
        parts.append(part)
        x = x - part.astype(F32)
    return parts


def mm(left, right):
    total = None
    most = max(len(left), len(right))
    for i, a in enumerate(left):
        for j, b in enumerate(right):
            if i + j < most:
                term = jnp.dot(a, b, preferred_element_type=F32)
                total = term if total is None else total + term
    return total


def kernel(
    sizes,
    inv_hbm, t_hbm, lead_l, lead_r, qw_hbm, slot_hbm, plane_hbm, dop_hbm, scr_hbm,
    dens_out, both_out,
    inv, t_ref, t_both, t_b, s_ref, k_ref, acc, e_ref, wire_in, wire_out, qw_ref, slot_ref, plane_ref,
    dopx, scrx, u1, u2, u3, part, zbuf, psrc, pbuf, mom, zmom, pmom, msrc,
    inv_sem, own_sem, halo_send, halo_recv, relay_send, relay_recv,
    zs, zr, ps, pr, mzs, mzr, mps, mpr,
):
    ny, nxl, nz, nxh, nc = sizes
    y, xl, z, xh, c = [lax.axis_index(a) for a in AXES]
    n_layer = nxh * nc
    n_plane = ny * nxl * n_layer
    n_energy = ny * nxl * nz
    layer = xh * nc + c
    energy = (y * nxl + xl) * nz + z
    slab = energy * n_layer + layer
    n_slabs = n_energy * n_layer
    here = (y * nxl + xl) * n_layer + layer
    count, size, _ = inv_hbm.shape
    planes = dop_hbm.shape[0]

    on_y, on_xl, on_z, on_xh, on_c = [
        [lax.rem(at + k, length) for k in range(length)] for at, length in zip((y, xl, z, xh, c), sizes)
    ]

    def around(k, length):
        return min(k, length - k)

    steps = sorted(
        itertools.product(range(ny), range(nxl), range(nxh), range(nc)),
        key=lambda k: -(around(k[0], ny) + k[1] + 2 * k[2]),
    )
    plane_peers = [
        (on_y[k[0]], on_xl[k[1]], z, on_xh[k[2]], on_c[k[3]]) for k in steps if any(k)
    ]
    line_peers = [(y, xl, on_z[k], xh, c) for k in sorted(range(1, nz), key=lambda k: -around(k, nz))]

    first = jnp.where(layer >= n_layer // 2, 1, 0)

    def layer_at(q, i):
        return q * (count - 1) + (1 - 2 * q) * i

    t_load = pltpu.make_async_copy(t_hbm, t_ref, own_sem.at[2])
    t_load.start()
    for i in range(count):
        l = layer_at(first, i)
        pltpu.make_async_copy(inv_hbm.at[l], inv.at[l], inv_sem.at[l]).start()
    lead_loads = [
        pltpu.make_async_copy(lead_l, e_ref.at[0], own_sem.at[3]),
        pltpu.make_async_copy(lead_r, e_ref.at[1], own_sem.at[4]),
    ]
    edges = [layer == 0, layer == n_layer - 1]
    for edge, copy in zip(edges, lead_loads):
        pl.when(edge)(copy.start)
    own = [
        pltpu.make_async_copy(dop_hbm, dopx.at[pl.ds(3, planes)], own_sem.at[0]),
        pltpu.make_async_copy(scr_hbm, scrx.at[pl.ds(2, planes)], own_sem.at[1]),
        pltpu.make_async_copy(qw_hbm, qw_ref, own_sem.at[5]),
        pltpu.make_async_copy(slot_hbm, slot_ref, own_sem.at[6]),
        pltpu.make_async_copy(plane_hbm, plane_ref, own_sem.at[7]),
    ]
    for copy in own:
        copy.start()

    def slab_dev(index):
        en, lay = lax.div(index, n_layer), lax.rem(index, n_layer)
        group, zz = lax.div(en, nz), lax.rem(en, nz)
        return (lax.div(group, nxl), lax.rem(group, nxl), zz, lax.div(lay, nc), lax.rem(lay, nc))

    slab_up = slab_dev(jnp.minimum(slab + 1, n_slabs - 1))
    slab_down = slab_dev(jnp.maximum(slab - 1, 0))

    barrier = pltpu.get_barrier_semaphore()
    extra_up = jnp.logical_and(layer == n_layer - 1, energy < n_energy - 1)
    extra_down = jnp.logical_and(layer == 0, energy > 0)
    for peer in line_peers + plane_peers:
        pl.semaphore_signal(barrier, inc=1, device_id=peer, device_id_type=MESH)

    @pl.when(extra_up)
    def _():
        pl.semaphore_signal(barrier, inc=1, device_id=slab_up, device_id_type=MESH)

    @pl.when(extra_down)
    def _():
        pl.semaphore_signal(barrier, inc=1, device_id=slab_down, device_id_type=MESH)

    t_load.wait()
    for q, value in enumerate((t_ref[...], t_ref[...].T)):
        t_both[q] = value
        t_b[q] = value.astype(BF16)

    rows = lax.broadcasted_iota(jnp.int32, (size, size), 0)
    cols = lax.broadcasted_iota(jnp.int32, (size, size), 1)

    def diagonal(mat):
        return jnp.sum(jnp.where(rows == cols, mat, 0.0), axis=0, keepdims=True)

    def propagator(q, i):
        d = inv[layer_at(q, i)]
        on = jnp.where(rows == cols, d, 0.0)
        down = jnp.sum(on, axis=1, keepdims=True)
        along = jnp.sum(on, axis=0, keepdims=True)
        off = [jnp.where(rows == cols, 0.0, d).astype(BF16)]
        p = down * t_both[q] + mm(off, [t_b[q]])
        pt = along * t_both[1 - q] + mm([t_b[1 - q]], off)
        return p, pt

    def pieces(p, pt):
        return parts_of(p, MOVE[0]), parts_of(pt, max(PULL[1], CARRY[1]))

    def begin(q):
        l = layer_at(q, 0)
        k = propagator(q, 0)[1]
        k_ref[q, l] = k
        return inv[l], k, pieces(*propagator(q, 1))

    def step(q, i, chain):
        s, k, (p, pt) = chain
        l = layer_at(q, i)
        y_mat = mm(parts_of(s, PULL[0]), pt[: PULL[1]])
        k = mm(parts_of(k, CARRY[0]), pt[: CARRY[1]])
        ahead = pieces(*propagator(q, i + 1)) if i + 1 < count else None
        moved = mm(p, parts_of(y_mat, MOVE[1]))
        k_ref[q, l] = k
        s = inv[l] + moved
        acc[pl.ds(l, 1), :] = acc[pl.ds(l, 1), :] + diagonal(moved)
        if i + 1 == count:
            s_ref[q] = s
        return s, k, ahead

    def halo_up():
        dev = slab_up
        return [
            pltpu.make_async_remote_copy(
                dop_hbm.at[pl.ds(planes - 3, 3)], dopx.at[pl.ds(0, 3)],
                halo_send.at[0], halo_recv.at[0], device_id=dev, device_id_type=MESH),
            pltpu.make_async_remote_copy(
                scr_hbm.at[pl.ds(planes - 2, 2)], scrx.at[pl.ds(0, 2)],
                halo_send.at[1], halo_recv.at[1], device_id=dev, device_id_type=MESH),
        ]

    def halo_down():
        dev = slab_down
        return [
            pltpu.make_async_remote_copy(
                dop_hbm.at[pl.ds(0, 3)], dopx.at[pl.ds(planes + 3, 3)],
                halo_send.at[2], halo_recv.at[2], device_id=dev, device_id_type=MESH),
            pltpu.make_async_remote_copy(
                scr_hbm.at[pl.ds(0, 2)], scrx.at[pl.ds(planes + 2, 2)],
                halo_send.at[3], halo_recv.at[3], device_id=dev, device_id_type=MESH),
        ]

    has_up = slab < n_slabs - 1
    has_down = slab > 0

    half = size // 2
    r_half = lax.broadcasted_iota(jnp.int32, (half, half), 0)
    c_half = lax.broadcasted_iota(jnp.int32, (half, half), 1)

    def pack(q, mat):
        one, two = mat[:half, :half], mat[half:, half:]
        wire_out[q, 0:half] = mat[:half, half:]
        wire_out[q, half:size] = jnp.where(r_half <= c_half, one, two)
        line = jnp.sum(jnp.where(r_half == c_half, two, 0.0), axis=0, keepdims=True)
        wire_out[q, size : size + 8] = jnp.broadcast_to(line, (8, half))

    def unpack(q):
        side, both = wire_in[q, 0:half], wire_in[q, half:size]
        over = both.T
        line = wire_in[q, size : size + 1]
        e_ref[q, 0:half, half:size] = side
        e_ref[q, half:size, 0:half] = side.T
        e_ref[q, 0:half, 0:half] = jnp.where(r_half <= c_half, both, over)
        two = jnp.where(r_half > c_half, both, over)
        e_ref[q, half:size, half:size] = jnp.where(r_half == c_half, line, two)

    def relay(q):
        to = jnp.clip(layer + 1 - 2 * q, 0, n_layer - 1)
        dev = (y, xl, z, lax.div(to, nc), lax.rem(to, nc))
        return pltpu.make_async_remote_copy(
            wire_out.at[q], wire_in.at[q], relay_send.at[q], relay_recv.at[q], device_id=dev, device_id_type=MESH
        )

    def row_of(q, eb, l):
        k_here = k_ref[q, l]
        g = mm(eb, parts_of(k_here, ENTER[1]))
        return k_here, g, jnp.sum(g * k_here, axis=0, keepdims=True)

    def add_row(l, row):
        acc[pl.ds(l, 1), :] = acc[pl.ds(l, 1), :] + row

    def pass_on(q):
        at_end = layer == (1 - q) * (n_layer - 1)
        l = layer_at(q, count - 1)
        k_last, g, row = row_of(q, parts_of(e_ref[q], ENTER[0]), l)

        @pl.when(jnp.logical_not(at_end))
        def _():
            pack(q, s_ref[q] + mm(parts_of(k_last.T, LEAVE[0]), parts_of(g, LEAVE[1])))
            relay(q).start()

        add_row(l, row)

    def rest(q):
        eb = parts_of(e_ref[q], ENTER[0])
        found = [row_of(q, eb, layer_at(q, i))[2] for i in range(count - 1)]
        for i, row in enumerate(found):
            add_row(layer_at(q, i), row)

    second = 1 - first
    for i in range(2):
        l = layer_at(first, i)
        pltpu.make_async_copy(inv_hbm.at[l], inv.at[l], inv_sem.at[l]).wait()
    def settle():
        for i in range(2, count):
            l = layer_at(first, i)
            pltpu.make_async_copy(inv_hbm.at[l], inv.at[l], inv_sem.at[l]).wait()
        for i in range(count):
            acc[i : i + 1, :] = diagonal(inv[i])

    def meet():
        more = jnp.where(extra_up, 1, 0) + jnp.where(extra_down, 1, 0)
        pl.semaphore_wait(barrier, nz - 1 + n_plane - 1 + more)

    def known(q):
        s = e_ref[q]
        ahead = pieces(*propagator(q, 0))
        settle()
        for i in range(count):
            p, pt = ahead
            l = layer_at(q, i)
            y_mat = mm(parts_of(s, PULL[0]), pt[: PULL[1]])
            ahead = pieces(*propagator(q, i + 1)) if i + 1 < count else None
            moved = mm(p, parts_of(y_mat, MOVE[1]))
            add_row(l, diagonal(moved))
            s = inv[l] + moved
        return s

    outer = jnp.logical_or(*edges)
    inner_seg = jnp.logical_not(outer)

    def start_halos():
        @pl.when(has_up)
        def _():
            for copy in halo_up():
                copy.start()

        @pl.when(has_down)
        def _():
            for copy in halo_down():
                copy.start()

    @pl.when(outer)
    def _():
        for edge, copy in zip(edges, lead_loads):
            pl.when(edge)(copy.wait)
        state = known(first)
        meet()
        pack(first, state)
        relay(first).start()

    @pl.when(inner_seg)
    def _():
        chain = begin(first)
        settle()
        for i in range(1, count):
            chain = step(first, i, chain)
        meet()

    chain = begin(second)
    for i in range(1, 1 + EARLY):
        chain = step(second, i, chain)

    @pl.when(inner_seg)
    def _():
        relay(first).wait_recv()
        unpack(first)
        pass_on(first)

    for i in range(1 + EARLY, count):
        chain = step(second, i, chain)

    start_halos()

    @pl.when(inner_seg)
    def _():
        rest(first)

    relay(second).wait_recv()
    unpack(second)
    pass_on(second)

    rest(second)

    for copy in own:
        copy.wait()
    slots = lax.broadcasted_iota(jnp.int32, qw_ref.shape, 1)
    weight = jnp.sum(jnp.where(slots == slot_ref[...], qw_ref[...], 0.0), axis=1, keepdims=True)
    part[...] = weight * acc[...]

    along_z = (z, line_peers)
    in_plane = (here, plane_peers)

    def exchange(group, src, buf, send, recv):
        me, peers = group
        for peer in peers:
            pltpu.make_async_remote_copy(
                src, buf.at[me], send, recv, device_id=peer, device_id_type=MESH
            ).start()
        buf[me] = src[...]
        all_of(group, src, buf, send, recv).wait_recv()

    def all_of(group, src, buf, send, recv):
        most = pl.ds(0, len(group[1]))
        return pltpu.make_async_remote_copy(
            buf.at[most], buf.at[most], send, recv, device_id=group[1][0], device_id_type=MESH
        )

    def total_of(buf, slots):
        total = None
        for k in slots:
            total = buf[k] if total is None else total + buf[k]
        return total

    exchange(along_z, part, zbuf, zs, zr)
    psrc[...] = total_of(zbuf, range(nz))
    exchange(in_plane, psrc, pbuf, ps, pr)
    gathered = [total_of(pbuf, range(lay, n_plane, n_layer)) for lay in range(n_layer)]
    dens = jnp.concatenate(gathered, axis=0)
    mine = gathered[0]
    for lay in range(1, n_layer):
        mine = jnp.where(layer == lay, gathered[lay], mine)
    dens_out[...] = mine

    @pl.when(has_down)
    def _():
        for copy in halo_up():
            copy.wait_recv()

    @pl.when(has_up)
    def _():
        for copy in halo_down():
            copy.wait_recv()

    @pl.when(jnp.logical_not(has_down))
    def _():
        dopx[0:3] = jnp.zeros((3, *dopx.shape[1:]), F32)
        scrx[0:2] = jnp.zeros((2, *scrx.shape[1:]), F32)

    @pl.when(jnp.logical_not(has_up))
    def _():
        dopx[planes + 3 : planes + 6] = jnp.zeros((3, *dopx.shape[1:]), F32)
        scrx[planes + 2 : planes + 4] = jnp.zeros((2, *scrx.shape[1:]), F32)

    low = slab * planes - 3
    n_near = planes + 6
    near = 16
    ids = low + lax.broadcasted_iota(jnp.int32, (near, plane_ref.shape[1]), 0)
    onehot = jnp.where(plane_ref[...] == ids, 1.0, 0.0)
    pc = jnp.dot(onehot, dens, precision=HI, preferred_element_type=F32)
    n_side = dop_hbm.shape[2]
    cell = n_side // ORB
    spread_m = lax.broadcasted_iota(jnp.int32, (size, n_side), 0)
    spread_z = lax.broadcasted_iota(jnp.int32, (size, n_side), 1)
    spread = jnp.where(lax.rem(spread_m, ORB) == lax.div(spread_z, cell), 1.0, 0.0)
    row_j = lax.broadcasted_iota(jnp.int32, (ORB, size), 0)
    row_m = lax.broadcasted_iota(jnp.int32, (ORB, size), 1)
    own_row = row_j == lax.div(row_m, ORB)
    tall = jnp.concatenate([jnp.where(own_row, pc[q : q + 1, :], 0.0) for q in range(n_near)], axis=0)
    wide = jnp.dot(tall, spread, precision=HI, preferred_element_type=F32)
    n_y = dop_hbm.shape[1]
    for q in range(n_near):
        for j in range(ORB):
            row = wide[q * ORB + j : q * ORB + j + 1, :]
            where = pl.ds(j * (n_y // ORB), n_y // ORB)
            dopx[q, where, :] = row - dopx[q, where, :]

    at_y = lax.broadcasted_iota(jnp.int32, (n_y, n_side), 0)
    at_z = lax.broadcasted_iota(jnp.int32, (n_y, n_side), 1)

    def applied(src, dst, trim):
        n_dst = n_near - 2 * trim
        for q in range(n_dst):
            mid = src[q + 1]
            beside = src[q] + src[q + 2]
            beside = beside + jnp.where(at_y == 0, 0.0, pltpu.roll(mid, 1, 0))
            beside = beside + jnp.where(at_y == n_y - 1, 0.0, pltpu.roll(mid, n_y - 1, 0))
            beside = beside + jnp.where(at_z == 0, 0.0, pltpu.roll(mid, 1, 1))
            beside = beside + jnp.where(at_z == n_side - 1, 0.0, pltpu.roll(mid, n_side - 1, 1))
            value = (scrx[q + trim - 1] + (6.0 - SHIFT)) * mid - beside
            if q < 3 - trim:
                value = jnp.where(has_down, value, 0.0)
            if q >= 3 - trim + planes:
                value = jnp.where(has_up, value, 0.0)
            dst[q] = value

    applied(dopx, u1, 1)
    applied(u1, u2, 2)
    applied(u2, u3, 3)

    def inner(a, a0, b, b0):
        total = None
        for q in range(planes):
            term = a[a0 + q] * b[b0 + q]
            total = term if total is None else total + term
        return jnp.sum(jnp.sum(total, axis=0, keepdims=True), axis=1, keepdims=True)

    sums = [
        inner(dopx, 3, dopx, 3), inner(dopx, 3, u1, 2), inner(u1, 2, u1, 2),
        inner(u1, 2, u2, 1), inner(u2, 1, u2, 1), inner(u2, 1, u3, 0),
    ]
    lane = lax.broadcasted_iota(jnp.int32, (1, 128), 1)
    row = jnp.zeros((1, 128), F32)
    for k, value in enumerate(sums):
        row = jnp.where(lane == k, value, row)
    mom[...] = row
    exchange(along_z, mom, zmom, mzs, mzr)
    msrc[...] = total_of(zmom, range(nz))
    exchange(in_plane, msrc, pmom, mps, mpr)
    total = total_of(pmom, range(n_plane))
    moment = [total[:, k : k + 1] for k in range(6)]

    def product(a, b):
        value = None
        for i, p in enumerate(a):
            for j, q in enumerate(b):
                term = p * q * moment[i + j]
                value = term if value is None else value + term
        return value

    def times_a(a):
        shifted = [None, *a]
        kept = [SHIFT * v for v in a] + [None]
        return [w if v is None else v if w is None else v + w for v, w in zip(shifted, kept)]

    def plus(a, factor, b):
        longest = max(len(a), len(b))
        result = []
        for i in range(longest):
            if i >= len(b):
                result.append(a[i])
            elif i >= len(a):
                result.append(factor * b[i])
            else:
                result.append(a[i] + factor * b[i])
        return result

    one = jnp.ones((1, 1), F32)
    residual, direction, potential = [one], [one], []
    norm = moment[0]
    for iteration in range(CG_ITERS):
        a_dir = times_a(direction)
        step_size = norm / product(direction, a_dir)
        potential = plus(potential, step_size, direction)
        residual = plus(residual, -step_size, a_dir)
        if iteration + 1 < CG_ITERS:
            new = product(residual, residual)
            direction = plus(residual, new / norm, direction)
            norm = new

    for q in range(planes):
        v = [dopx[3 + q], u1[2 + q], u2[1 + q], u3[q]]
        x = potential[0] * v[0]
        for k in range(1, CG_ITERS):
            x = x + potential[k] * v[k]
        both_out[0, q] = x
        r = residual[0] * v[0]
        for k in range(1, CG_ITERS + 1):
            r = r + residual[k] * v[k]
        both_out[1, q] = r

    for sent in (
        (along_z, part, zbuf, zs, zr), (in_plane, psrc, pbuf, ps, pr),
        (along_z, mom, zmom, mzs, mzr), (in_plane, msrc, pmom, mps, mpr),
    ):
        all_of(*sent).wait_send()

    relay(first).wait_send()

    @pl.when(inner_seg)
    def _():
        relay(second).wait_send()

    @pl.when(has_up)
    def _():
        for copy in halo_up():
            copy.wait_send()

    @pl.when(has_down)
    def _():
        for copy in halo_down():
            copy.wait_send()


def body(
    sizes,
    layer_inverse,
    coupling,
    lead_left,
    lead_right,
    quad_weight,
    energy_slot,
    plane_of,
    doping,
    screening,
):
    ny, nxl, nz, nxh, nc = sizes
    _, count, size, _ = layer_inverse.shape
    planes, n_y, n_z = doping.shape
    n_plane = ny * nxl * nxh * nc
    vmem = pl.BlockSpec(memory_space=pltpu.VMEM)
    hbm = pl.BlockSpec(memory_space=pltpu.HBM)
    square = pltpu.VMEM((size, size), F32)
    squares = pltpu.VMEM((count, size, size), F32)
    dma = pltpu.SemaphoreType.DMA
    rows = pltpu.VMEM((count, size), F32)
    operands = (
        layer_inverse[0], coupling, lead_left[0], lead_right[0], quad_weight[None], energy_slot[None], plane_of[None],
        doping, screening,
    )
    dens, both = pl.pallas_call(
        functools.partial(kernel, sizes),
        out_shape=(
            jax.ShapeDtypeStruct((count, size), F32),
            jax.ShapeDtypeStruct((2, *doping.shape), F32),
        ),
        in_specs=[hbm] * 9,
        out_specs=(vmem, vmem),
        scratch_shapes=[
            squares,
            square,
            pltpu.VMEM((2, size, size), F32),
            pltpu.VMEM((2, size, size), BF16),
            pltpu.VMEM((2, size, size), F32),
            pltpu.VMEM((2, count, size, size), F32),
            rows,
            pltpu.VMEM((2, size, size), F32),
            pltpu.VMEM((2, size + 8, size // 2), F32),
            pltpu.VMEM((2, size + 8, size // 2), F32),
            pltpu.VMEM((1, quad_weight.shape[0]), F32),
            pltpu.VMEM((1, 1), jnp.int32),
            pltpu.VMEM((1, plane_of.shape[0]), jnp.int32),
            pltpu.VMEM((planes + 6, n_y, n_z), F32),
            pltpu.VMEM((planes + 4, n_y, n_z), F32),
            pltpu.VMEM((planes + 4, n_y, n_z), F32),
            pltpu.VMEM((planes + 2, n_y, n_z), F32),
            pltpu.VMEM((planes, n_y, n_z), F32),
            rows,
            pltpu.VMEM((nz, count, size), F32),
            rows,
            pltpu.VMEM((n_plane, count, size), F32),
            pltpu.VMEM((1, 128), F32),
            pltpu.VMEM((nz, 1, 128), F32),
            pltpu.VMEM((n_plane, 1, 128), F32),
            pltpu.VMEM((1, 128), F32),
            dma((count,)), dma((8,)), dma((4,)), dma((4,)), dma((2,)), dma((2,)),
            *[dma] * 8,
        ],
        compiler_params=pltpu.CompilerParams(
            collective_id=0, has_side_effects=True, vmem_limit_bytes=VMEM
        ),
    )(*[v if v.size == 1 else pltpu.with_memory_space_constraint(v, pltpu.HBM) for v in operands])
    return dens, both[0], both[1]


def sharded(split):
    energy_layer = (*ENERGY, *LAYER)
    in_specs = (
        P(ENERGY, LAYER, None, None),
        P(),
        P(ENERGY, None, None),
        P(ENERGY, None, None),
        P(),
        P(ENERGY),
        P(),
        P(energy_layer, None, None),
        P(energy_layer, None, None),
    )
    out_specs = (P(LAYER, None), P(energy_layer, None, None), P(energy_layer, None, None))
    sizes = tuple(split.shape[a] for a in AXES)
    return jax.shard_map(
        functools.partial(body, sizes), mesh=split, in_specs=in_specs, out_specs=out_specs, check_vma=False
    )


def solution(mesh):
    return sharded(Mesh(mesh.devices.reshape(4, 2, 8, 2, 2), AXES))
```

```python
import functools
import itertools

import jax
import jax.numpy as jnp
from jax import lax
from jax.experimental import pallas as pl
from jax.experimental.pallas import tpu as pltpu
from jax.sharding import Mesh
from jax.sharding import PartitionSpec as P

AXES = ("energy_0", "energy_1", "energy_2", "layer_0", "layer_1")
LAYER = ("layer_0", "layer_1")
ENERGY = ("energy_0", "energy_1", "energy_2")
ORB = 16
CG_ITERS = 3
SHIFT = 7.0
VMEM = 48 * 1024 * 1024
PULL = (1, 2)
CARRY = (1, 2)
MOVE = (2, 1)
ENTER = (1, 1)
LEAVE = (1, 1)
EARLY = 1
MESH = pl.DeviceIdType.MESH
HI = lax.Precision.HIGHEST
F32 = jnp.float32
BF16 = jnp.bfloat16


def parts_of(x, count):
    parts = []
    for _ in range(count):
        part = x.astype(BF16)
        parts.append(part)
        x = x - part.astype(F32)
    return parts


def mm(left, right):
    total = None
    most = max(len(left), len(right))
    for i, a in enumerate(left):
        for j, b in enumerate(right):
            if i + j < most:
                term = jnp.dot(a, b, preferred_element_type=F32)
                total = term if total is None else total + term
    return total


def kernel(
    sizes,
    inv_hbm, t_hbm, lead_l, lead_r, qw_hbm, slot_hbm, plane_hbm, dop_hbm, scr_hbm,
    dens_out, both_out,
    inv, t_ref, t_both, t_b, s_ref, k_ref, acc, e_ref, wire_in, wire_out, qw_ref, slot_ref, plane_ref,
    dopx, scrx, u1, u2, u3, part, zbuf, psrc, pbuf, mom, amom,
    inv_sem, own_sem, halo_send, halo_recv, relay_send, relay_recv,
    zs, zr, ps, pr, mas, mar,
):
    ny, nxl, nz, nxh, nc = sizes
    y, xl, z, xh, c = [lax.axis_index(a) for a in AXES]
    n_layer = nxh * nc
    n_plane = ny * nxl * n_layer
    n_energy = ny * nxl * nz
    layer = xh * nc + c
    energy = (y * nxl + xl) * nz + z
    slab = energy * n_layer + layer
    n_slabs = n_energy * n_layer
    here = (y * nxl + xl) * n_layer + layer
    count, size, _ = inv_hbm.shape
    planes = dop_hbm.shape[0]

    on_y, on_xl, on_z, on_xh, on_c = [
        [lax.rem(at + k, length) for k in range(length)] for at, length in zip((y, xl, z, xh, c), sizes)
    ]

    def around(k, length):
        return min(k, length - k)

    steps = sorted(
        itertools.product(range(ny), range(nxl), range(nxh), range(nc)),
        key=lambda k: -(around(k[0], ny) + k[1] + 2 * k[2]),
    )
    plane_peers = [
        (on_y[k[0]], on_xl[k[1]], z, on_xh[k[2]], on_c[k[3]]) for k in steps if any(k)
    ]
    line_peers = [(y, xl, on_z[k], xh, c) for k in sorted(range(1, nz), key=lambda k: -around(k, nz))]

    first = jnp.where(layer >= n_layer // 2, 1, 0)

    def layer_at(q, i):
        return q * (count - 1) + (1 - 2 * q) * i

    t_load = pltpu.make_async_copy(t_hbm, t_ref, own_sem.at[2])
    t_load.start()
    for i in range(count):
        l = layer_at(first, i)
        pltpu.make_async_copy(inv_hbm.at[l], inv.at[l], inv_sem.at[l]).start()
    lead_loads = [
        pltpu.make_async_copy(lead_l, e_ref.at[0], own_sem.at[3]),
        pltpu.make_async_copy(lead_r, e_ref.at[1], own_sem.at[4]),
    ]
    edges = [layer == 0, layer == n_layer - 1]
    for edge, copy in zip(edges, lead_loads):
        pl.when(edge)(copy.start)
    own = [
        pltpu.make_async_copy(dop_hbm, dopx.at[pl.ds(3, planes)], own_sem.at[0]),
        pltpu.make_async_copy(scr_hbm, scrx.at[pl.ds(2, planes)], own_sem.at[1]),
        pltpu.make_async_copy(qw_hbm, qw_ref, own_sem.at[5]),
        pltpu.make_async_copy(slot_hbm, slot_ref, own_sem.at[6]),
        pltpu.make_async_copy(plane_hbm, plane_ref, own_sem.at[7]),
    ]
    for copy in own:
        copy.start()

    everywhere = sorted(
        itertools.product(range(ny), range(nxl), range(nz), range(nxh), range(nc)),
        key=lambda k: -(around(k[0], ny) + k[1] + around(k[2], nz) + 2 * k[3]),
    )
    all_peers = [(on_y[k[0]], on_xl[k[1]], on_z[k[2]], on_xh[k[3]], on_c[k[4]]) for k in everywhere if any(k)]

    def slab_dev(index):
        en, lay = lax.div(index, n_layer), lax.rem(index, n_layer)
        group, zz = lax.div(en, nz), lax.rem(en, nz)
        return (lax.div(group, nxl), lax.rem(group, nxl), zz, lax.div(lay, nc), lax.rem(lay, nc))

    slab_up = slab_dev(jnp.minimum(slab + 1, n_slabs - 1))
    slab_down = slab_dev(jnp.maximum(slab - 1, 0))

    barrier = pltpu.get_barrier_semaphore()
    extra_up = jnp.logical_and(layer == n_layer - 1, energy < n_energy - 1)
    extra_down = jnp.logical_and(layer == 0, energy > 0)
    for peer in line_peers + plane_peers:
        pl.semaphore_signal(barrier, inc=1, device_id=peer, device_id_type=MESH)

    @pl.when(extra_up)
    def _():
        pl.semaphore_signal(barrier, inc=1, device_id=slab_up, device_id_type=MESH)

    @pl.when(extra_down)
    def _():
        pl.semaphore_signal(barrier, inc=1, device_id=slab_down, device_id_type=MESH)

    t_load.wait()
    for q, value in enumerate((t_ref[...], t_ref[...].T)):
        t_both[q] = value
        t_b[q] = value.astype(BF16)

    rows = lax.broadcasted_iota(jnp.int32, (size, size), 0)
    cols = lax.broadcasted_iota(jnp.int32, (size, size), 1)

    def diagonal(mat):
        return jnp.sum(jnp.where(rows == cols, mat, 0.0), axis=0, keepdims=True)

    def propagator(q, i):
        d = inv[layer_at(q, i)]
        on = jnp.where(rows == cols, d, 0.0)
        down = jnp.sum(on, axis=1, keepdims=True)
        along = jnp.sum(on, axis=0, keepdims=True)
        off = [jnp.where(rows == cols, 0.0, d).astype(BF16)]
        p = down * t_both[q] + mm(off, [t_b[q]])
        pt = along * t_both[1 - q] + mm([t_b[1 - q]], off)
        return p, pt

    def pieces(p, pt):
        return parts_of(p, MOVE[0]), parts_of(pt, max(PULL[1], CARRY[1]))

    def begin(q):
        l = layer_at(q, 0)
        k = propagator(q, 0)[1]
        k_ref[q, l] = k
        return inv[l], k, pieces(*propagator(q, 1))

    def step(q, i, chain):
        s, k, (p, pt) = chain
        l = layer_at(q, i)
        y_mat = mm(parts_of(s, PULL[0]), pt[: PULL[1]])
        k = mm(parts_of(k, CARRY[0]), pt[: CARRY[1]])
        ahead = pieces(*propagator(q, i + 1)) if i + 1 < count else None
        moved = mm(p, parts_of(y_mat, MOVE[1]))
        k_ref[q, l] = k
        s = inv[l] + moved
        acc[pl.ds(l, 1), :] = acc[pl.ds(l, 1), :] + diagonal(moved)
        if i + 1 == count:
            s_ref[q] = s
        return s, k, ahead

    def halo_up():
        dev = slab_up
        return [
            pltpu.make_async_remote_copy(
                dop_hbm.at[pl.ds(planes - 3, 3)], dopx.at[pl.ds(0, 3)],
                halo_send.at[0], halo_recv.at[0], device_id=dev, device_id_type=MESH),
            pltpu.make_async_remote_copy(
                scr_hbm.at[pl.ds(planes - 2, 2)], scrx.at[pl.ds(0, 2)],
                halo_send.at[1], halo_recv.at[1], device_id=dev, device_id_type=MESH),
        ]

    def halo_down():
        dev = slab_down
        return [
            pltpu.make_async_remote_copy(
                dop_hbm.at[pl.ds(0, 3)], dopx.at[pl.ds(planes + 3, 3)],
                halo_send.at[2], halo_recv.at[2], device_id=dev, device_id_type=MESH),
            pltpu.make_async_remote_copy(
                scr_hbm.at[pl.ds(0, 2)], scrx.at[pl.ds(planes + 2, 2)],
                halo_send.at[3], halo_recv.at[3], device_id=dev, device_id_type=MESH),
        ]

    has_up = slab < n_slabs - 1
    has_down = slab > 0

    half = size // 2
    r_half = lax.broadcasted_iota(jnp.int32, (half, half), 0)
    c_half = lax.broadcasted_iota(jnp.int32, (half, half), 1)

    def pack(q, mat):
        one, two = mat[:half, :half], mat[half:, half:]
        wire_out[q, 0:half] = mat[:half, half:]
        wire_out[q, half:size] = jnp.where(r_half <= c_half, one, two)
        line = jnp.sum(jnp.where(r_half == c_half, two, 0.0), axis=0, keepdims=True)
        wire_out[q, size : size + 8] = jnp.broadcast_to(line, (8, half))

    def unpack(q):
        side, both = wire_in[q, 0:half], wire_in[q, half:size]
        over = both.T
        line = wire_in[q, size : size + 1]
        e_ref[q, 0:half, half:size] = side
        e_ref[q, half:size, 0:half] = side.T
        e_ref[q, 0:half, 0:half] = jnp.where(r_half <= c_half, both, over)
        two = jnp.where(r_half > c_half, both, over)
        e_ref[q, half:size, half:size] = jnp.where(r_half == c_half, line, two)

    def relay(q):
        to = jnp.clip(layer + 1 - 2 * q, 0, n_layer - 1)
        dev = (y, xl, z, lax.div(to, nc), lax.rem(to, nc))
        return pltpu.make_async_remote_copy(
            wire_out.at[q], wire_in.at[q], relay_send.at[q], relay_recv.at[q], device_id=dev, device_id_type=MESH
        )

    def row_of(q, eb, l):
        k_here = k_ref[q, l]
        g = mm(eb, parts_of(k_here, ENTER[1]))
        return k_here, g, jnp.sum(g * k_here, axis=0, keepdims=True)

    def add_row(l, row):
        acc[pl.ds(l, 1), :] = acc[pl.ds(l, 1), :] + row

    def pass_on(q):
        at_end = layer == (1 - q) * (n_layer - 1)
        l = layer_at(q, count - 1)
        k_last, g, row = row_of(q, parts_of(e_ref[q], ENTER[0]), l)

        @pl.when(jnp.logical_not(at_end))
        def _():
            pack(q, s_ref[q] + mm(parts_of(k_last.T, LEAVE[0]), parts_of(g, LEAVE[1])))
            relay(q).start()

        add_row(l, row)

    def rest(q):
        eb = parts_of(e_ref[q], ENTER[0])
        found = [row_of(q, eb, layer_at(q, i))[2] for i in range(count - 1)]
        for i, row in enumerate(found):
            add_row(layer_at(q, i), row)

    second = 1 - first
    for i in range(2):
        l = layer_at(first, i)
        pltpu.make_async_copy(inv_hbm.at[l], inv.at[l], inv_sem.at[l]).wait()
    def settle():
        for i in range(2, count):
            l = layer_at(first, i)
            pltpu.make_async_copy(inv_hbm.at[l], inv.at[l], inv_sem.at[l]).wait()
        for i in range(count):
            acc[i : i + 1, :] = diagonal(inv[i])

    def meet():
        more = jnp.where(extra_up, 1, 0) + jnp.where(extra_down, 1, 0)
        pl.semaphore_wait(barrier, nz - 1 + n_plane - 1 + more)

    def known(q):
        s = e_ref[q]
        ahead = pieces(*propagator(q, 0))
        settle()
        for i in range(count):
            p, pt = ahead
            l = layer_at(q, i)
            y_mat = mm(parts_of(s, PULL[0]), pt[: PULL[1]])
            ahead = pieces(*propagator(q, i + 1)) if i + 1 < count else None
            moved = mm(p, parts_of(y_mat, MOVE[1]))
            add_row(l, diagonal(moved))
            s = inv[l] + moved
        return s

    outer = jnp.logical_or(*edges)
    inner_seg = jnp.logical_not(outer)

    def start_halos():
        @pl.when(has_up)
        def _():
            for copy in halo_up():
                copy.start()

        @pl.when(has_down)
        def _():
            for copy in halo_down():
                copy.start()

    @pl.when(outer)
    def _():
        for edge, copy in zip(edges, lead_loads):
            pl.when(edge)(copy.wait)
        state = known(first)
        meet()
        pack(first, state)
        relay(first).start()

    @pl.when(inner_seg)
    def _():
        chain = begin(first)
        settle()
        for i in range(1, count):
            chain = step(first, i, chain)
        meet()

    chain = begin(second)
    for i in range(1, 1 + EARLY):
        chain = step(second, i, chain)

    @pl.when(inner_seg)
    def _():
        relay(first).wait_recv()
        unpack(first)
        pass_on(first)

    for i in range(1 + EARLY, count):
        chain = step(second, i, chain)

    start_halos()

    @pl.when(inner_seg)
    def _():
        rest(first)

    relay(second).wait_recv()
    unpack(second)
    pass_on(second)

    rest(second)

    for copy in own:
        copy.wait()
    slots = lax.broadcasted_iota(jnp.int32, qw_ref.shape, 1)
    weight = jnp.sum(jnp.where(slots == slot_ref[...], qw_ref[...], 0.0), axis=1, keepdims=True)
    part[...] = weight * acc[...]

    along_z = (z, line_peers)
    in_plane = (here, plane_peers)
    over_all = (slab, all_peers)

    def exchange(group, src, buf, send, recv):
        me, peers = group
        for peer in peers:
            pltpu.make_async_remote_copy(
                src, buf.at[me], send, recv, device_id=peer, device_id_type=MESH
            ).start()
        buf[me] = src[...]
        all_of(group, src, buf, send, recv).wait_recv()

    def all_of(group, src, buf, send, recv):
        most = pl.ds(0, len(group[1]))
        return pltpu.make_async_remote_copy(
            buf.at[most], buf.at[most], send, recv, device_id=group[1][0], device_id_type=MESH
        )

    def total_of(buf, slots):
        total = None
        for k in slots:
            total = buf[k] if total is None else total + buf[k]
        return total

    exchange(along_z, part, zbuf, zs, zr)
    psrc[...] = total_of(zbuf, range(nz))
    exchange(in_plane, psrc, pbuf, ps, pr)
    gathered = [total_of(pbuf, range(lay, n_plane, n_layer)) for lay in range(n_layer)]
    dens = jnp.concatenate(gathered, axis=0)
    mine = gathered[0]
    for lay in range(1, n_layer):
        mine = jnp.where(layer == lay, gathered[lay], mine)
    dens_out[...] = mine

    @pl.when(has_down)
    def _():
        for copy in halo_up():
            copy.wait_recv()

    @pl.when(has_up)
    def _():
        for copy in halo_down():
            copy.wait_recv()

    @pl.when(jnp.logical_not(has_down))
    def _():
        dopx[0:3] = jnp.zeros((3, *dopx.shape[1:]), F32)
        scrx[0:2] = jnp.zeros((2, *scrx.shape[1:]), F32)

    @pl.when(jnp.logical_not(has_up))
    def _():
        dopx[planes + 3 : planes + 6] = jnp.zeros((3, *dopx.shape[1:]), F32)
        scrx[planes + 2 : planes + 4] = jnp.zeros((2, *scrx.shape[1:]), F32)

    low = slab * planes - 3
    n_near = planes + 6
    near = 16
    ids = low + lax.broadcasted_iota(jnp.int32, (near, plane_ref.shape[1]), 0)
    onehot = jnp.where(plane_ref[...] == ids, 1.0, 0.0)
    pc = jnp.dot(onehot, dens, precision=HI, preferred_element_type=F32)
    n_side = dop_hbm.shape[2]
    cell = n_side // ORB
    spread_m = lax.broadcasted_iota(jnp.int32, (size, n_side), 0)
    spread_z = lax.broadcasted_iota(jnp.int32, (size, n_side), 1)
    spread = jnp.where(lax.rem(spread_m, ORB) == lax.div(spread_z, cell), 1.0, 0.0)
    row_j = lax.broadcasted_iota(jnp.int32, (ORB, size), 0)
    row_m = lax.broadcasted_iota(jnp.int32, (ORB, size), 1)
    own_row = row_j == lax.div(row_m, ORB)
    tall = jnp.concatenate([jnp.where(own_row, pc[q : q + 1, :], 0.0) for q in range(n_near)], axis=0)
    wide = jnp.dot(tall, spread, precision=HI, preferred_element_type=F32)
    n_y = dop_hbm.shape[1]
    for q in range(n_near):
        for j in range(ORB):
            row = wide[q * ORB + j : q * ORB + j + 1, :]
            where = pl.ds(j * (n_y // ORB), n_y // ORB)
            dopx[q, where, :] = row - dopx[q, where, :]

    at_y = lax.broadcasted_iota(jnp.int32, (n_y, n_side), 0)
    at_z = lax.broadcasted_iota(jnp.int32, (n_y, n_side), 1)

    def applied(src, dst, trim):
        n_dst = n_near - 2 * trim
        for q in range(n_dst):
            mid = src[q + 1]
            beside = src[q] + src[q + 2]
            beside = beside + jnp.where(at_y == 0, 0.0, pltpu.roll(mid, 1, 0))
            beside = beside + jnp.where(at_y == n_y - 1, 0.0, pltpu.roll(mid, n_y - 1, 0))
            beside = beside + jnp.where(at_z == 0, 0.0, pltpu.roll(mid, 1, 1))
            beside = beside + jnp.where(at_z == n_side - 1, 0.0, pltpu.roll(mid, n_side - 1, 1))
            value = (scrx[q + trim - 1] + (6.0 - SHIFT)) * mid - beside
            if q < 3 - trim:
                value = jnp.where(has_down, value, 0.0)
            if q >= 3 - trim + planes:
                value = jnp.where(has_up, value, 0.0)
            dst[q] = value

    applied(dopx, u1, 1)
    applied(u1, u2, 2)
    applied(u2, u3, 3)

    def inner(a, a0, b, b0):
        total = None
        for q in range(planes):
            term = a[a0 + q] * b[b0 + q]
            total = term if total is None else total + term
        return jnp.sum(jnp.sum(total, axis=0, keepdims=True), axis=1, keepdims=True)

    sums = [
        inner(dopx, 3, dopx, 3), inner(dopx, 3, u1, 2), inner(u1, 2, u1, 2),
        inner(u1, 2, u2, 1), inner(u2, 1, u2, 1), inner(u2, 1, u3, 0),
    ]
    lane = lax.broadcasted_iota(jnp.int32, (1, 128), 1)
    row = jnp.zeros((1, 128), F32)
    for k, value in enumerate(sums):
        row = jnp.where(lane == k, value, row)
    mom[...] = row
    exchange(over_all, mom, amom, mas, mar)
    totals = [total_of(amom, range(k, n_slabs, 8)) for k in range(8)]
    total = sum(totals[1:], totals[0])
    moment = [total[:, k : k + 1] for k in range(6)]

    def product(a, b):
        value = None
        for i, p in enumerate(a):
            for j, q in enumerate(b):
                term = p * q * moment[i + j]
                value = term if value is None else value + term
        return value

    def times_a(a):
        shifted = [None, *a]
        kept = [SHIFT * v for v in a] + [None]
        return [w if v is None else v if w is None else v + w for v, w in zip(shifted, kept)]

    def plus(a, factor, b):
        longest = max(len(a), len(b))
        result = []
        for i in range(longest):
            if i >= len(b):
                result.append(a[i])
            elif i >= len(a):
                result.append(factor * b[i])
            else:
                result.append(a[i] + factor * b[i])
        return result

    one = jnp.ones((1, 1), F32)
    residual, direction, potential = [one], [one], []
    norm = moment[0]
    for iteration in range(CG_ITERS):
        a_dir = times_a(direction)
        step_size = norm / product(direction, a_dir)
        potential = plus(potential, step_size, direction)
        residual = plus(residual, -step_size, a_dir)
        if iteration + 1 < CG_ITERS:
            new = product(residual, residual)
            direction = plus(residual, new / norm, direction)
            norm = new

    for q in range(planes):
        v = [dopx[3 + q], u1[2 + q], u2[1 + q], u3[q]]
        x = potential[0] * v[0]
        for k in range(1, CG_ITERS):
            x = x + potential[k] * v[k]
        both_out[0, q] = x
        r = residual[0] * v[0]
        for k in range(1, CG_ITERS + 1):
            r = r + residual[k] * v[k]
        both_out[1, q] = r

    for sent in (
        (along_z, part, zbuf, zs, zr), (in_plane, psrc, pbuf, ps, pr),
        (over_all, mom, amom, mas, mar),
    ):
        all_of(*sent).wait_send()

    relay(first).wait_send()

    @pl.when(inner_seg)
    def _():
        relay(second).wait_send()

    @pl.when(has_up)
    def _():
        for copy in halo_up():
            copy.wait_send()

    @pl.when(has_down)
    def _():
        for copy in halo_down():
            copy.wait_send()


def body(
    sizes,
    layer_inverse,
    coupling,
    lead_left,
    lead_right,
    quad_weight,
    energy_slot,
    plane_of,
    doping,
    screening,
):
    ny, nxl, nz, nxh, nc = sizes
    _, count, size, _ = layer_inverse.shape
    planes, n_y, n_z = doping.shape
    n_plane = ny * nxl * nxh * nc
    vmem = pl.BlockSpec(memory_space=pltpu.VMEM)
    hbm = pl.BlockSpec(memory_space=pltpu.HBM)
    square = pltpu.VMEM((size, size), F32)
    squares = pltpu.VMEM((count, size, size), F32)
    dma = pltpu.SemaphoreType.DMA
    rows = pltpu.VMEM((count, size), F32)
    operands = (
        layer_inverse[0], coupling, lead_left[0], lead_right[0], quad_weight[None], energy_slot[None], plane_of[None],
        doping, screening,
    )
    dens, both = pl.pallas_call(
        functools.partial(kernel, sizes),
        out_shape=(
            jax.ShapeDtypeStruct((count, size), F32),
            jax.ShapeDtypeStruct((2, *doping.shape), F32),
        ),
        in_specs=[hbm] * 9,
        out_specs=(vmem, vmem),
        scratch_shapes=[
            squares,
            square,
            pltpu.VMEM((2, size, size), F32),
            pltpu.VMEM((2, size, size), BF16),
            pltpu.VMEM((2, size, size), F32),
            pltpu.VMEM((2, count, size, size), F32),
            rows,
            pltpu.VMEM((2, size, size), F32),
            pltpu.VMEM((2, size + 8, size // 2), F32),
            pltpu.VMEM((2, size + 8, size // 2), F32),
            pltpu.VMEM((1, quad_weight.shape[0]), F32),
            pltpu.VMEM((1, 1), jnp.int32),
            pltpu.VMEM((1, plane_of.shape[0]), jnp.int32),
            pltpu.VMEM((planes + 6, n_y, n_z), F32),
            pltpu.VMEM((planes + 4, n_y, n_z), F32),
            pltpu.VMEM((planes + 4, n_y, n_z), F32),
            pltpu.VMEM((planes + 2, n_y, n_z), F32),
            pltpu.VMEM((planes, n_y, n_z), F32),
            rows,
            pltpu.VMEM((nz, count, size), F32),
            rows,
            pltpu.VMEM((n_plane, count, size), F32),
            pltpu.VMEM((1, 128), F32),
            pltpu.VMEM((n_plane * nz, 1, 128), F32),
            dma((count,)), dma((8,)), dma((4,)), dma((4,)), dma((2,)), dma((2,)),
            *[dma] * 6,
        ],
        compiler_params=pltpu.CompilerParams(
            collective_id=0, has_side_effects=True, vmem_limit_bytes=VMEM
        ),
    )(*[v if v.size == 1 else pltpu.with_memory_space_constraint(v, pltpu.HBM) for v in operands])
    return dens, both[0], both[1]


def sharded(split):
    energy_layer = (*ENERGY, *LAYER)
    in_specs = (
        P(ENERGY, LAYER, None, None),
        P(),
        P(ENERGY, None, None),
        P(ENERGY, None, None),
        P(),
        P(ENERGY),
        P(),
        P(energy_layer, None, None),
        P(energy_layer, None, None),
    )
    out_specs = (P(LAYER, None), P(energy_layer, None, None), P(energy_layer, None, None))
    sizes = tuple(split.shape[a] for a in AXES)
    return jax.shard_map(
        functools.partial(body, sizes), mesh=split, in_specs=in_specs, out_specs=out_specs, check_vma=False
    )


def solution(mesh):
    return sharded(Mesh(mesh.devices.reshape(4, 2, 8, 2, 2), AXES))
```

```python
import functools
import itertools

import jax
import jax.numpy as jnp
from jax import lax
from jax.experimental import pallas as pl
from jax.experimental.pallas import tpu as pltpu
from jax.sharding import Mesh
from jax.sharding import PartitionSpec as P

AXES = ("energy_0", "energy_1", "energy_2", "layer_0", "layer_1")
LAYER = ("layer_0", "layer_1")
ENERGY = ("energy_0", "energy_1", "energy_2")
ORB = 16
CG_ITERS = 3
SHIFT = 7.0
VMEM = 48 * 1024 * 1024
PULL = (1, 2)
CARRY = (1, 2)
MOVE = (2, 1)
ENTER = (1, 1)
LEAVE = (1, 1)
EARLY = 1
MESH = pl.DeviceIdType.MESH
HI = lax.Precision.HIGHEST
F32 = jnp.float32
BF16 = jnp.bfloat16


def parts_of(x, count):
    parts = []
    for _ in range(count):
        part = x.astype(BF16)
        parts.append(part)
        x = x - part.astype(F32)
    return parts


def mm(left, right):
    total = None
    most = max(len(left), len(right))
    for i, a in enumerate(left):
        for j, b in enumerate(right):
            if i + j < most:
                term = jnp.dot(a, b, preferred_element_type=F32)
                total = term if total is None else total + term
    return total


def kernel(
    sizes,
    inv_hbm, t_hbm, lead_l, lead_r, qw_hbm, slot_hbm, plane_hbm, dop_hbm, scr_hbm,
    dens_out, both_out,
    inv, t_ref, t_both, t_b, s_ref, k_ref, acc, e_ref, wire_in, wire_out, qw_ref, slot_ref, plane_ref, onehot_ref, spread_ref,
    dopx, scrx, u1, u2, u3, part, zbuf, psrc, pbuf, mom, amom,
    inv_sem, own_sem, halo_send, halo_recv, relay_send, relay_recv,
    zs, zr, ps, pr, mas, mar,
):
    ny, nxl, nz, nxh, nc = sizes
    y, xl, z, xh, c = [lax.axis_index(a) for a in AXES]
    n_layer = nxh * nc
    n_plane = ny * nxl * n_layer
    n_energy = ny * nxl * nz
    layer = xh * nc + c
    energy = (y * nxl + xl) * nz + z
    slab = energy * n_layer + layer
    n_slabs = n_energy * n_layer
    here = (y * nxl + xl) * n_layer + layer
    count, size, _ = inv_hbm.shape
    planes = dop_hbm.shape[0]

    on_y, on_xl, on_z, on_xh, on_c = [
        [lax.rem(at + k, length) for k in range(length)] for at, length in zip((y, xl, z, xh, c), sizes)
    ]

    def around(k, length):
        return min(k, length - k)

    steps = sorted(
        itertools.product(range(ny), range(nxl), range(nxh), range(nc)),
        key=lambda k: -(around(k[0], ny) + k[1] + 2 * k[2]),
    )
    plane_peers = [
        (on_y[k[0]], on_xl[k[1]], z, on_xh[k[2]], on_c[k[3]]) for k in steps if any(k)
    ]
    line_peers = [(y, xl, on_z[k], xh, c) for k in sorted(range(1, nz), key=lambda k: -around(k, nz))]

    first = jnp.where(layer >= n_layer // 2, 1, 0)

    def layer_at(q, i):
        return q * (count - 1) + (1 - 2 * q) * i

    t_load = pltpu.make_async_copy(t_hbm, t_ref, own_sem.at[2])
    t_load.start()
    for i in range(count):
        l = layer_at(first, i)
        pltpu.make_async_copy(inv_hbm.at[l], inv.at[l], inv_sem.at[l]).start()
    lead_loads = [
        pltpu.make_async_copy(lead_l, e_ref.at[0], own_sem.at[3]),
        pltpu.make_async_copy(lead_r, e_ref.at[1], own_sem.at[4]),
    ]
    edges = [layer == 0, layer == n_layer - 1]
    for edge, copy in zip(edges, lead_loads):
        pl.when(edge)(copy.start)
    own = [
        pltpu.make_async_copy(dop_hbm, dopx.at[pl.ds(3, planes)], own_sem.at[0]),
        pltpu.make_async_copy(scr_hbm, scrx.at[pl.ds(2, planes)], own_sem.at[1]),
        pltpu.make_async_copy(qw_hbm, qw_ref, own_sem.at[5]),
        pltpu.make_async_copy(slot_hbm, slot_ref, own_sem.at[6]),
        pltpu.make_async_copy(plane_hbm, plane_ref, own_sem.at[7]),
    ]
    for copy in own:
        copy.start()

    everywhere = sorted(
        itertools.product(range(ny), range(nxl), range(nz), range(nxh), range(nc)),
        key=lambda k: -(around(k[0], ny) + k[1] + around(k[2], nz) + 2 * k[3]),
    )
    all_peers = [(on_y[k[0]], on_xl[k[1]], on_z[k[2]], on_xh[k[3]], on_c[k[4]]) for k in everywhere if any(k)]

    def slab_dev(index):
        en, lay = lax.div(index, n_layer), lax.rem(index, n_layer)
        group, zz = lax.div(en, nz), lax.rem(en, nz)
        return (lax.div(group, nxl), lax.rem(group, nxl), zz, lax.div(lay, nc), lax.rem(lay, nc))

    slab_up = slab_dev(jnp.minimum(slab + 1, n_slabs - 1))
    slab_down = slab_dev(jnp.maximum(slab - 1, 0))

    barrier = pltpu.get_barrier_semaphore()
    extra_up = jnp.logical_and(layer == n_layer - 1, energy < n_energy - 1)
    extra_down = jnp.logical_and(layer == 0, energy > 0)
    for peer in line_peers + plane_peers:
        pl.semaphore_signal(barrier, inc=1, device_id=peer, device_id_type=MESH)

    @pl.when(extra_up)
    def _():
        pl.semaphore_signal(barrier, inc=1, device_id=slab_up, device_id_type=MESH)

    @pl.when(extra_down)
    def _():
        pl.semaphore_signal(barrier, inc=1, device_id=slab_down, device_id_type=MESH)

    t_load.wait()
    for q, value in enumerate((t_ref[...], t_ref[...].T)):
        t_both[q] = value
        t_b[q] = value.astype(BF16)

    rows = lax.broadcasted_iota(jnp.int32, (size, size), 0)
    cols = lax.broadcasted_iota(jnp.int32, (size, size), 1)

    def diagonal(mat):
        return jnp.sum(jnp.where(rows == cols, mat, 0.0), axis=0, keepdims=True)

    def propagator(q, i):
        d = inv[layer_at(q, i)]
        on = jnp.where(rows == cols, d, 0.0)
        down = jnp.sum(on, axis=1, keepdims=True)
        along = jnp.sum(on, axis=0, keepdims=True)
        off = [jnp.where(rows == cols, 0.0, d).astype(BF16)]
        p = down * t_both[q] + mm(off, [t_b[q]])
        pt = along * t_both[1 - q] + mm([t_b[1 - q]], off)
        return p, pt

    def pieces(p, pt):
        return parts_of(p, MOVE[0]), parts_of(pt, max(PULL[1], CARRY[1]))

    def begin(q):
        l = layer_at(q, 0)
        k = propagator(q, 0)[1]
        k_ref[q, l] = k
        return inv[l], k, pieces(*propagator(q, 1))

    def step(q, i, chain):
        s, k, (p, pt) = chain
        l = layer_at(q, i)
        y_mat = mm(parts_of(s, PULL[0]), pt[: PULL[1]])
        k = mm(parts_of(k, CARRY[0]), pt[: CARRY[1]])
        ahead = pieces(*propagator(q, i + 1)) if i + 1 < count else None
        moved = mm(p, parts_of(y_mat, MOVE[1]))
        k_ref[q, l] = k
        s = inv[l] + moved
        acc[pl.ds(l, 1), :] = acc[pl.ds(l, 1), :] + diagonal(moved)
        if i + 1 == count:
            s_ref[q] = s
        return s, k, ahead

    def halo_up():
        dev = slab_up
        return [
            pltpu.make_async_remote_copy(
                dop_hbm.at[pl.ds(planes - 3, 3)], dopx.at[pl.ds(0, 3)],
                halo_send.at[0], halo_recv.at[0], device_id=dev, device_id_type=MESH),
            pltpu.make_async_remote_copy(
                scr_hbm.at[pl.ds(planes - 2, 2)], scrx.at[pl.ds(0, 2)],
                halo_send.at[1], halo_recv.at[1], device_id=dev, device_id_type=MESH),
        ]

    def halo_down():
        dev = slab_down
        return [
            pltpu.make_async_remote_copy(
                dop_hbm.at[pl.ds(0, 3)], dopx.at[pl.ds(planes + 3, 3)],
                halo_send.at[2], halo_recv.at[2], device_id=dev, device_id_type=MESH),
            pltpu.make_async_remote_copy(
                scr_hbm.at[pl.ds(0, 2)], scrx.at[pl.ds(planes + 2, 2)],
                halo_send.at[3], halo_recv.at[3], device_id=dev, device_id_type=MESH),
        ]

    has_up = slab < n_slabs - 1
    has_down = slab > 0

    half = size // 2
    r_half = lax.broadcasted_iota(jnp.int32, (half, half), 0)
    c_half = lax.broadcasted_iota(jnp.int32, (half, half), 1)

    def pack(q, mat):
        one, two = mat[:half, :half], mat[half:, half:]
        wire_out[q, 0:half] = mat[:half, half:]
        wire_out[q, half:size] = jnp.where(r_half <= c_half, one, two)
        line = jnp.sum(jnp.where(r_half == c_half, two, 0.0), axis=0, keepdims=True)
        wire_out[q, size : size + 8] = jnp.broadcast_to(line, (8, half))

    def unpack(q):
        side, both = wire_in[q, 0:half], wire_in[q, half:size]
        over = both.T
        line = wire_in[q, size : size + 1]
        e_ref[q, 0:half, half:size] = side
        e_ref[q, half:size, 0:half] = side.T
        e_ref[q, 0:half, 0:half] = jnp.where(r_half <= c_half, both, over)
        two = jnp.where(r_half > c_half, both, over)
        e_ref[q, half:size, half:size] = jnp.where(r_half == c_half, line, two)

    def relay(q):
        to = jnp.clip(layer + 1 - 2 * q, 0, n_layer - 1)
        dev = (y, xl, z, lax.div(to, nc), lax.rem(to, nc))
        return pltpu.make_async_remote_copy(
            wire_out.at[q], wire_in.at[q], relay_send.at[q], relay_recv.at[q], device_id=dev, device_id_type=MESH
        )

    def row_of(q, eb, l):
        k_here = k_ref[q, l]
        g = mm(eb, parts_of(k_here, ENTER[1]))
        return k_here, g, jnp.sum(g * k_here, axis=0, keepdims=True)

    def add_row(l, row):
        acc[pl.ds(l, 1), :] = acc[pl.ds(l, 1), :] + row

    def pass_on(q):
        at_end = layer == (1 - q) * (n_layer - 1)
        l = layer_at(q, count - 1)
        k_last, g, row = row_of(q, parts_of(e_ref[q], ENTER[0]), l)

        @pl.when(jnp.logical_not(at_end))
        def _():
            pack(q, s_ref[q] + mm(parts_of(k_last.T, LEAVE[0]), parts_of(g, LEAVE[1])))
            relay(q).start()

        add_row(l, row)

    def rest(q):
        eb = parts_of(e_ref[q], ENTER[0])
        found = [row_of(q, eb, layer_at(q, i))[2] for i in range(count - 1)]
        for i, row in enumerate(found):
            add_row(layer_at(q, i), row)

    second = 1 - first
    for i in range(2):
        l = layer_at(first, i)
        pltpu.make_async_copy(inv_hbm.at[l], inv.at[l], inv_sem.at[l]).wait()
    def settle():
        for i in range(2, count):
            l = layer_at(first, i)
            pltpu.make_async_copy(inv_hbm.at[l], inv.at[l], inv_sem.at[l]).wait()
        for i in range(count):
            acc[i : i + 1, :] = diagonal(inv[i])

    def meet():
        more = jnp.where(extra_up, 1, 0) + jnp.where(extra_down, 1, 0)
        pl.semaphore_wait(barrier, nz - 1 + n_plane - 1 + more)

    def known(q):
        s = e_ref[q]
        ahead = pieces(*propagator(q, 0))
        settle()
        for i in range(count):
            p, pt = ahead
            l = layer_at(q, i)
            y_mat = mm(parts_of(s, PULL[0]), pt[: PULL[1]])
            ahead = pieces(*propagator(q, i + 1)) if i + 1 < count else None
            moved = mm(p, parts_of(y_mat, MOVE[1]))
            add_row(l, diagonal(moved))
            s = inv[l] + moved
        return s

    outer = jnp.logical_or(*edges)
    inner_seg = jnp.logical_not(outer)

    def start_halos():
        @pl.when(has_up)
        def _():
            for copy in halo_up():
                copy.start()

        @pl.when(has_down)
        def _():
            for copy in halo_down():
                copy.start()

    @pl.when(outer)
    def _():
        for edge, copy in zip(edges, lead_loads):
            pl.when(edge)(copy.wait)
        state = known(first)
        meet()
        pack(first, state)
        relay(first).start()

    @pl.when(inner_seg)
    def _():
        chain = begin(first)
        settle()
        for i in range(1, count):
            chain = step(first, i, chain)
        meet()

    chain = begin(second)
    for i in range(1, 1 + EARLY):
        chain = step(second, i, chain)

    @pl.when(inner_seg)
    def _():
        relay(first).wait_recv()
        unpack(first)
        pass_on(first)

    for i in range(1 + EARLY, count):
        chain = step(second, i, chain)

    start_halos()

    @pl.when(inner_seg)
    def _():
        rest(first)

    for copy in own:
        copy.wait()
    slots = lax.broadcasted_iota(jnp.int32, qw_ref.shape, 1)
    weight = jnp.sum(jnp.where(slots == slot_ref[...], qw_ref[...], 0.0), axis=1, keepdims=True)
    low = slab * planes - 3
    n_near = planes + 6
    near = 16
    ids = low + lax.broadcasted_iota(jnp.int32, (near, plane_ref.shape[1]), 0)
    onehot_ref[...] = jnp.where(plane_ref[...] == ids, 1.0, 0.0)
    n_side = dop_hbm.shape[2]
    cell = n_side // ORB
    spread_m = lax.broadcasted_iota(jnp.int32, (size, n_side), 0)
    spread_z = lax.broadcasted_iota(jnp.int32, (size, n_side), 1)
    spread_ref[...] = jnp.where(lax.rem(spread_m, ORB) == lax.div(spread_z, cell), 1.0, 0.0)
    row_j = lax.broadcasted_iota(jnp.int32, (ORB, size), 0)
    row_m = lax.broadcasted_iota(jnp.int32, (ORB, size), 1)
    own_row = row_j == lax.div(row_m, ORB)
    relay(second).wait_recv()
    unpack(second)
    pass_on(second)

    rest(second)

    part[...] = weight * acc[...]

    along_z = (z, line_peers)
    in_plane = (here, plane_peers)
    over_all = (slab, all_peers)

    def exchange(group, src, buf, send, recv):
        me, peers = group
        for peer in peers:
            pltpu.make_async_remote_copy(
                src, buf.at[me], send, recv, device_id=peer, device_id_type=MESH
            ).start()
        buf[me] = src[...]
        all_of(group, src, buf, send, recv).wait_recv()

    def all_of(group, src, buf, send, recv):
        most = pl.ds(0, len(group[1]))
        return pltpu.make_async_remote_copy(
            buf.at[most], buf.at[most], send, recv, device_id=group[1][0], device_id_type=MESH
        )

    def total_of(buf, slots):
        total = None
        for k in slots:
            total = buf[k] if total is None else total + buf[k]
        return total

    exchange(along_z, part, zbuf, zs, zr)
    psrc[...] = total_of(zbuf, range(nz))
    exchange(in_plane, psrc, pbuf, ps, pr)
    gathered = [total_of(pbuf, range(lay, n_plane, n_layer)) for lay in range(n_layer)]
    dens = jnp.concatenate(gathered, axis=0)
    mine = gathered[0]
    for lay in range(1, n_layer):
        mine = jnp.where(layer == lay, gathered[lay], mine)
    dens_out[...] = mine

    @pl.when(has_down)
    def _():
        for copy in halo_up():
            copy.wait_recv()

    @pl.when(has_up)
    def _():
        for copy in halo_down():
            copy.wait_recv()

    @pl.when(jnp.logical_not(has_down))
    def _():
        dopx[0:3] = jnp.zeros((3, *dopx.shape[1:]), F32)
        scrx[0:2] = jnp.zeros((2, *scrx.shape[1:]), F32)

    @pl.when(jnp.logical_not(has_up))
    def _():
        dopx[planes + 3 : planes + 6] = jnp.zeros((3, *dopx.shape[1:]), F32)
        scrx[planes + 2 : planes + 4] = jnp.zeros((2, *scrx.shape[1:]), F32)

    pc = jnp.dot(onehot_ref[...], dens, precision=HI, preferred_element_type=F32)
    tall = jnp.concatenate([jnp.where(own_row, pc[q : q + 1, :], 0.0) for q in range(n_near)], axis=0)
    wide = jnp.dot(tall, spread_ref[...], precision=HI, preferred_element_type=F32)
    n_y = dop_hbm.shape[1]
    for q in range(n_near):
        for j in range(ORB):
            row = wide[q * ORB + j : q * ORB + j + 1, :]
            where = pl.ds(j * (n_y // ORB), n_y // ORB)
            dopx[q, where, :] = row - dopx[q, where, :]

    at_y = lax.broadcasted_iota(jnp.int32, (n_y, n_side), 0)
    at_z = lax.broadcasted_iota(jnp.int32, (n_y, n_side), 1)

    def applied(src, dst, trim):
        n_dst = n_near - 2 * trim
        for q in range(n_dst):
            mid = src[q + 1]
            beside = src[q] + src[q + 2]
            beside = beside + jnp.where(at_y == 0, 0.0, pltpu.roll(mid, 1, 0))
            beside = beside + jnp.where(at_y == n_y - 1, 0.0, pltpu.roll(mid, n_y - 1, 0))
            beside = beside + jnp.where(at_z == 0, 0.0, pltpu.roll(mid, 1, 1))
            beside = beside + jnp.where(at_z == n_side - 1, 0.0, pltpu.roll(mid, n_side - 1, 1))
            value = (scrx[q + trim - 1] + (6.0 - SHIFT)) * mid - beside
            if q < 3 - trim:
                value = jnp.where(has_down, value, 0.0)
            if q >= 3 - trim + planes:
                value = jnp.where(has_up, value, 0.0)
            dst[q] = value

    applied(dopx, u1, 1)
    applied(u1, u2, 2)
    applied(u2, u3, 3)

    def inner(a, a0, b, b0):
        total = None
        for q in range(planes):
            term = a[a0 + q] * b[b0 + q]
            total = term if total is None else total + term
        return jnp.sum(jnp.sum(total, axis=0, keepdims=True), axis=1, keepdims=True)

    sums = [
        inner(dopx, 3, dopx, 3), inner(dopx, 3, u1, 2), inner(u1, 2, u1, 2),
        inner(u1, 2, u2, 1), inner(u2, 1, u2, 1), inner(u2, 1, u3, 0),
    ]
    lane = lax.broadcasted_iota(jnp.int32, (1, 128), 1)
    row = jnp.zeros((1, 128), F32)
    for k, value in enumerate(sums):
        row = jnp.where(lane == k, value, row)
    mom[...] = row
    exchange(over_all, mom, amom, mas, mar)
    totals = [total_of(amom, range(k, n_slabs, 8)) for k in range(8)]
    total = sum(totals[1:], totals[0])
    moment = [total[:, k : k + 1] for k in range(6)]

    def product(a, b):
        value = None
        for i, p in enumerate(a):
            for j, q in enumerate(b):
                term = p * q * moment[i + j]
                value = term if value is None else value + term
        return value

    def times_a(a):
        shifted = [None, *a]
        kept = [SHIFT * v for v in a] + [None]
        return [w if v is None else v if w is None else v + w for v, w in zip(shifted, kept)]

    def plus(a, factor, b):
        longest = max(len(a), len(b))
        result = []
        for i in range(longest):
            if i >= len(b):
                result.append(a[i])
            elif i >= len(a):
                result.append(factor * b[i])
            else:
                result.append(a[i] + factor * b[i])
        return result

    one = jnp.ones((1, 1), F32)
    residual, direction, potential = [one], [one], []
    norm = moment[0]
    for iteration in range(CG_ITERS):
        a_dir = times_a(direction)
        step_size = norm / product(direction, a_dir)
        potential = plus(potential, step_size, direction)
        residual = plus(residual, -step_size, a_dir)
        if iteration + 1 < CG_ITERS:
            new = product(residual, residual)
            direction = plus(residual, new / norm, direction)
            norm = new

    for q in range(planes):
        v = [dopx[3 + q], u1[2 + q], u2[1 + q], u3[q]]
        x = potential[0] * v[0]
        for k in range(1, CG_ITERS):
            x = x + potential[k] * v[k]
        both_out[0, q] = x
        r = residual[0] * v[0]
        for k in range(1, CG_ITERS + 1):
            r = r + residual[k] * v[k]
        both_out[1, q] = r

    for sent in (
        (along_z, part, zbuf, zs, zr), (in_plane, psrc, pbuf, ps, pr),
        (over_all, mom, amom, mas, mar),
    ):
        all_of(*sent).wait_send()

    relay(first).wait_send()

    @pl.when(inner_seg)
    def _():
        relay(second).wait_send()

    @pl.when(has_up)
    def _():
        for copy in halo_up():
            copy.wait_send()

    @pl.when(has_down)
    def _():
        for copy in halo_down():
            copy.wait_send()


def body(
    sizes,
    layer_inverse,
    coupling,
    lead_left,
    lead_right,
    quad_weight,
    energy_slot,
    plane_of,
    doping,
    screening,
):
    ny, nxl, nz, nxh, nc = sizes
    _, count, size, _ = layer_inverse.shape
    planes, n_y, n_z = doping.shape
    n_plane = ny * nxl * nxh * nc
    vmem = pl.BlockSpec(memory_space=pltpu.VMEM)
    hbm = pl.BlockSpec(memory_space=pltpu.HBM)
    square = pltpu.VMEM((size, size), F32)
    squares = pltpu.VMEM((count, size, size), F32)
    dma = pltpu.SemaphoreType.DMA
    rows = pltpu.VMEM((count, size), F32)
    operands = (
        layer_inverse[0], coupling, lead_left[0], lead_right[0], quad_weight[None], energy_slot[None], plane_of[None],
        doping, screening,
    )
    dens, both = pl.pallas_call(
        functools.partial(kernel, sizes),
        out_shape=(
            jax.ShapeDtypeStruct((count, size), F32),
            jax.ShapeDtypeStruct((2, *doping.shape), F32),
        ),
        in_specs=[hbm] * 9,
        out_specs=(vmem, vmem),
        scratch_shapes=[
            squares,
            square,
            pltpu.VMEM((2, size, size), F32),
            pltpu.VMEM((2, size, size), BF16),
            pltpu.VMEM((2, size, size), F32),
            pltpu.VMEM((2, count, size, size), F32),
            rows,
            pltpu.VMEM((2, size, size), F32),
            pltpu.VMEM((2, size + 8, size // 2), F32),
            pltpu.VMEM((2, size + 8, size // 2), F32),
            pltpu.VMEM((1, quad_weight.shape[0]), F32),
            pltpu.VMEM((1, 1), jnp.int32),
            pltpu.VMEM((1, plane_of.shape[0]), jnp.int32),
            pltpu.VMEM((16, plane_of.shape[0]), F32),
            pltpu.VMEM((size, n_z), F32),
            pltpu.VMEM((planes + 6, n_y, n_z), F32),
            pltpu.VMEM((planes + 4, n_y, n_z), F32),
            pltpu.VMEM((planes + 4, n_y, n_z), F32),
            pltpu.VMEM((planes + 2, n_y, n_z), F32),
            pltpu.VMEM((planes, n_y, n_z), F32),
            rows,
            pltpu.VMEM((nz, count, size), F32),
            rows,
            pltpu.VMEM((n_plane, count, size), F32),
            pltpu.VMEM((1, 128), F32),
            pltpu.VMEM((n_plane * nz, 1, 128), F32),
            dma((count,)), dma((8,)), dma((4,)), dma((4,)), dma((2,)), dma((2,)),
            *[dma] * 6,
        ],
        compiler_params=pltpu.CompilerParams(
            collective_id=0, has_side_effects=True, vmem_limit_bytes=VMEM
        ),
    )(*[v if v.size == 1 else pltpu.with_memory_space_constraint(v, pltpu.HBM) for v in operands])
    return dens, both[0], both[1]


def sharded(split):
    energy_layer = (*ENERGY, *LAYER)
    in_specs = (
        P(ENERGY, LAYER, None, None),
        P(),
        P(ENERGY, None, None),
        P(ENERGY, None, None),
        P(),
        P(ENERGY),
        P(),
        P(energy_layer, None, None),
        P(energy_layer, None, None),
    )
    out_specs = (P(LAYER, None), P(energy_layer, None, None), P(energy_layer, None, None))
    sizes = tuple(split.shape[a] for a in AXES)
    return jax.shard_map(
        functools.partial(body, sizes), mesh=split, in_specs=in_specs, out_specs=out_specs, check_vma=False
    )


def solution(mesh):
    return sharded(Mesh(mesh.devices.reshape(4, 2, 8, 2, 2), AXES))
```
